32 devices in a mesh: wide: 16 (over z, x, core), narrow: 2 (over y).
Axes of the slice: x: 2, y: 2, z: 4, core: 2. Of those that a mesh axis runs over, the one named last changes fastest.
Arguments:
- diffusivity: float32 [64, 16, 256], P('wide', None, 'narrow'), may hold values from 0.06 to 0.13
- velocity: float32 [64, 16, 256], P('wide', None, 'narrow'), may hold values from 0 to 0.9
- damping: float32 [64, 16, 256], P('wide', None, 'narrow'), may hold values from 0.02 to 0.2
- input_amplitude: float32 [64, 64, 256], P(None, 'wide', 'narrow'), may hold values from -6 to 6
- output_amplitude: float32 [64, 64, 256], P(None, 'wide', 'narrow'), may hold values from -6 to 6
- input_height: int32 [64], replicated, may hold values from 0 to 15
- output_height: int32 [64], replicated, may hold values from 0 to 15
- start_block: float32 [64, 32], replicated, may hold values from -0.75 to 0.75
Outputs:
- direct_modes: float32 [32, 64, 16, 256], P(None, 'wide', None, 'narrow')
- adjoint_modes: float32 [32, 64, 16, 256], P(None, 'wide', None, 'narrow')
The draws below stay inside these ranges and needn't reach their ends.
Inputs may be any that keep to these rules, and one draw needn't show every extreme that they name: Input j forces only the wall-parallel plane at wall-normal index input_height[j]. Output k weights only the wall-parallel plane at wall-normal index output_height[k].
All inputs are finite; a program needn't handle non-finite values.
Results may differ from the reference program's by a relative error of at most 0.0003.
Values sent between devices are 32-bit elements; how exact they have to be, the bound alone decides.
No kernel may reach another device: no remote copies, remote signals or barrier semaphores. Data moves between devices by JAX's collectives and lax.ppermute only.
A program may use at most 128 MiB of HBM per device.

```python
import math
import jax
import jax.numpy as jnp
from jax import lax

INPUTS = 64
RANK = 32
STEPS = 4
NY = 16
NX = 64
NZ = 256


def set_ends(array, key, least, largest):
    shape = array.shape
    spot = [jax.random.randint(jax.random.fold_in(key, axis), (), 0, shape[axis]) for axis in range(len(shape))]
    array = array.at[tuple(spot)].set(least)
    longest = shape.index(max(shape))
    spot[longest] = (spot[longest] + 1) % shape[longest]
    return array.at[tuple(spot)].set(largest)


def steps_of(key, shape, cuts, least, largest):
    factor_of = 1.0
    for axis_at, parts in cuts:
        draws = jax.random.uniform(jax.random.fold_in(jax.random.fold_in(key, 6), axis_at), (parts,), jnp.float32, least / len(cuts), largest / len(cuts))
        factor_of = factor_of * jnp.repeat(jnp.exp(draws), shape[axis_at] // parts).reshape((-1,) + (1,) * (len(shape) - 1 - axis_at))
    return factor_of


def centred(rng, shape, scale, limit, cuts=(), held_as=jnp.bfloat16):
    level = steps_of(rng, shape, cuts, -0.22, 0.18) if cuts else 1.0
    drawn = jax.random.normal(rng, shape, jnp.float32) * scale * level
    return jnp.minimum(jnp.maximum(drawn, -limit), limit).astype(held_as)


def setup_inputs(seed: int = 0) -> dict:
    splits = jax.random.split(jax.random.key(seed), 9)
    diffusivity = jnp.clip(0.06 + 0.06999999657273293 * jax.random.uniform(splits[0], (NX, NY, NZ), jnp.float32) ** steps_of(splits[0], (NX, NY, NZ), ((0, 16), (2, 2)), -0.2, 0.2), 0.06, 0.13)
    velocity = jnp.clip(0.9 * jax.random.uniform(splits[1], (NX, NY, NZ), jnp.float32) ** steps_of(splits[1], (NX, NY, NZ), ((0, 16), (2, 2)), -0.2, 0.2), 0.0, 0.9)
    damping = jnp.clip(jnp.exp(math.log(0.2) - 2.3025851 * jax.random.uniform(splits[2], (NX, NY, NZ), jnp.float32) ** steps_of(splits[2], (NX, NY, NZ), ((0, 16), (2, 2)), -0.2, 0.2)), 0.02, 0.2)
    input_amplitude = centred(splits[3], (INPUTS, NX, NZ), 1.0, 6.0, ((1, 16), (2, 2)), jnp.float32)
    output_amplitude = centred(splits[4], (INPUTS, NX, NZ), 1.0, 6.0, ((1, 16), (2, 2)), jnp.float32)
    input_height = set_ends(jax.random.randint(splits[5], (INPUTS,), 0, NY), jax.random.fold_in(splits[5], 1), 0, NY - 1).astype(jnp.int32)
    output_height = set_ends(jax.random.randint(splits[6], (INPUTS,), 0, NY), jax.random.fold_in(splits[6], 1), 0, NY - 1).astype(jnp.int32)
    start_block = centred(splits[7], (INPUTS, RANK), INPUTS ** -0.5, 0.75, (), jnp.float32)
    return dict(diffusivity=diffusivity, velocity=velocity, damping=damping, input_amplitude=input_amplitude, output_amplitude=output_amplitude, input_height=input_height, output_height=output_height, start_block=start_block)


HIGH = lax.Precision.HIGHEST

def direct_step(field, center, back, front, kappa):
    padded = jnp.pad(field, ((0, 0), (1, 1), (1, 1), (1, 1)))
    core = padded[:, 1:-1, 1:-1, 1:-1]
    wall = padded[:, 1:-1, :-2, 1:-1] + padded[:, 1:-1, 2:, 1:-1]
    beside = wall + padded[:, 1:-1, 1:-1, :-2] + padded[:, 1:-1, 1:-1, 2:]
    return center * core + back * padded[:, :-2, 1:-1, 1:-1] + front * padded[:, 2:, 1:-1, 1:-1] + kappa * beside

def adjoint_step(field, center, back, front, kappa):
    pads = ((0, 0), (1, 1), (1, 1), (1, 1))
    carried_back = jnp.pad(back * field, pads)
    carried_front = jnp.pad(front * field, pads)
    spread = jnp.pad(kappa * field, pads)
    wall = spread[:, 1:-1, :-2, 1:-1] + spread[:, 1:-1, 2:, 1:-1]
    beside = wall + spread[:, 1:-1, 1:-1, :-2] + spread[:, 1:-1, 1:-1, 2:]
    return center * field + carried_back[:, 2:, 1:-1, 1:-1] + carried_front[:, :-2, 1:-1, 1:-1] + beside

def march(amplitude, height, coefs, stepper):
    levels = jnp.arange(NY, dtype=jnp.int32)
    picked = (levels[None, :] == height[:, None]).astype(jnp.float32)
    field = amplitude[:, :, None, :] * picked[:, None, :, None]
    for step in range(STEPS):
        field = stepper(field, *coefs)
    return field

def orthonormal(block):
    lower = jnp.linalg.cholesky(jnp.dot(block.T, block, precision=HIGH))
    basis = lax.linalg.triangular_solve(lower, block.T, left_side=True, lower=True).T
    return (basis, lower)

def balance(gram, start_block):
    first, unused = orthonormal(jnp.dot(gram, start_block, precision=HIGH))
    right, unused = orthonormal(jnp.dot(gram.T, first, precision=HIGH))
    left, lower = orthonormal(jnp.dot(gram, right, precision=HIGH))
    roots = jnp.sqrt(jnp.diagonal(lower))
    direct_mix = lax.linalg.triangular_solve(lower, right.T, left_side=True, lower=True).T * roots[None, :]
    adjoint_mix = left / roots[None, :]
    return (direct_mix, adjoint_mix)

def reference(diffusivity, velocity, damping, input_amplitude, output_amplitude, input_height, output_height, start_block):
    center = 1.0 - 6.0 * diffusivity - damping
    back = diffusivity * (1.0 + velocity)
    front = diffusivity * (1.0 - velocity)
    coefs = (center, back, front, diffusivity)
    blocks = INPUTS // 8

    def run(stepper, amplitude, height):
        pieces = lax.map(lambda item: march(item[0], item[1], coefs, stepper), (amplitude.reshape(blocks, 8, NX, NZ), height.reshape(blocks, 8)))
        return pieces.reshape(INPUTS, NX * NY * NZ)
    direct_flat = run(direct_step, input_amplitude, input_height)
    adjoint_flat = run(adjoint_step, output_amplitude, output_height)
    gram = jnp.dot(adjoint_flat.astype(jnp.float32), direct_flat.T.astype(jnp.float32), precision=HIGH, preferred_element_type=jnp.float32)
    gram = gram * (1.0 / math.sqrt(NX * NY * NZ))
    direct_mix, adjoint_mix = balance(gram, start_block)
    direct_modes = jnp.dot(direct_mix.T, direct_flat, precision=HIGH).reshape(RANK, NX, NY, NZ)
    adjoint_modes = jnp.dot(adjoint_mix.T, adjoint_flat, precision=HIGH).reshape(RANK, NX, NY, NZ)
    return (direct_modes, adjoint_modes)
```

```python
import functools
import math

import jax
import jax.numpy as jnp
from jax import lax
from jax.experimental import pallas as pl
from jax.experimental.pallas import tpu as pltpu
from jax.sharding import PartitionSpec as P

STEPS = 4
HIGH = lax.Precision.HIGHEST
LANES = 128
SUB = 8
SLOT = 32
PER = LANES // SLOT
LEFT = 0
RIGHT = 16
REACH = STEPS + SUB

VMEM = pl.BlockSpec(memory_space=pltpu.VMEM)
SMEM = pl.BlockSpec(memory_space=pltpu.SMEM)


def swaps(count):
    near = [(i, i ^ 1) for i in range(count) if i ^ 1 < count]
    far = [(i, ((i + 1) ^ 1) - 1) for i in range(count) if 0 <= ((i + 1) ^ 1) - 1 < count]
    return near, far


def lane_ids(shape):
    return lax.broadcasted_iota(jnp.int32, shape, len(shape) - 1)


def turn(value, amount):
    return pltpu.roll(value, amount % LANES, value.ndim - 1)


def edges(block, slot):
    within = lane_ids(block.shape) - slot * SLOT
    low = turn(block, slot * SLOT + LEFT + STEPS)
    high = turn(block, slot * SLOT + RIGHT - (LANES - SUB))
    is_low = (within >= LEFT + STEPS) & (within < LEFT + REACH)
    is_high = (within >= RIGHT) & (within < RIGHT + SUB)
    return jnp.where(is_low, low, jnp.where(is_high, high, 0.0))


def pack_kernel(
    inputs, width_x, depth_y, place_ref, rank_ref,
    amp_in, amp_out, diff, vel, damp, near, far,
    sorted_ref, cell_ref, rim_ref,
):
    own = width_x
    near_x = place_ref[0]
    far_x = place_ref[1]
    for system, source in ((0, amp_in), (1, amp_out)):
        base = system * inputs * width_x

        def move(j, carry, system=system, source=source, base=base):
            to = rank_ref[system, j]
            for x in range(width_x):
                sorted_ref[system, own + x, pl.ds(to, 1), :] = source[pl.ds(j * width_x + x, 1), :]
                row = base + j * width_x + x
                sorted_ref[system, near_x + x, pl.ds(to, 1), :] = near[pl.ds(row, 1), :]
                sorted_ref[system, far_x + x, pl.ds(to, 1), :] = far[pl.ds(row, 1), :]
            return carry

        lax.fori_loop(0, inputs, move, 0, unroll=4)
    start = 2 * inputs * width_x
    for which, source in enumerate((diff, vel, damp)):
        for x in range(width_x):
            rows = pl.ds(start + (which * width_x + x) * depth_y, depth_y)
            cell_ref[which, own + x] = source[x]
            cell_ref[which, near_x + x] = near[rows, :]
            cell_ref[which, far_x + x] = far[rows, :]
    groups = inputs // SUB
    rims = groups // PER
    extent = 3 * width_x
    tiles = depth_y // SUB

    def rim_row(x, carry):
        for system in range(2):
            for rim in range(rims):
                total = jnp.zeros((SUB, LANES), jnp.float32)
                for slot in range(PER):
                    group = rim * PER + slot
                    total = total + edges(sorted_ref[system, x, group * SUB : (group + 1) * SUB, :], slot)
                rim_ref[(system * rims + rim) * extent + x] = total
        pieces = [(which, tile) for which in range(3) for tile in range(tiles)]
        for at in range(0, len(pieces), PER):
            total = jnp.zeros((SUB, LANES), jnp.float32)
            for slot, (which, tile) in enumerate(pieces[at : at + PER]):
                total = total + edges(cell_ref[which, x, tile * SUB : (tile + 1) * SUB, :], slot)
            rim_ref[(2 * rims + at // PER) * extent + x] = total
        return carry

    lax.fori_loop(0, extent, rim_row, 0)


def split(value):
    first = value.astype(jnp.bfloat16)
    rest = value - first.astype(jnp.float32)
    second = rest.astype(jnp.bfloat16)
    third = (rest - second.astype(jnp.float32)).astype(jnp.bfloat16)
    return first, second, third


def window_kernel(
    inputs, width_x, depth_y, bounds_ref, flag_ref,
    sorted_ref, cell_ref, rim_ref, from_right, from_left, level_ref,
    direct_ref, adjoint_ref, gram_ref,
    amp, coef, ping, pong, field, total_ref,
):
    groups = inputs // SUB
    rims = groups // PER
    extent = 3 * width_x
    tiles = depth_y // SUB
    lanes = lane_ids((SUB, LANES))
    within = lanes % SLOT
    from_right_lane = (within >= RIGHT + SUB) & (within < RIGHT + REACH) & (flag_ref[0] > 0)
    from_left_lane = (within >= LEFT) & (within < LEFT + STEPS) & (flag_ref[1] > 0)

    def whole_rim(index):
        value = rim_ref[index]
        value = jnp.where(from_right_lane, turn(from_right[index], RIGHT + SUB - STEPS), value)
        return jnp.where(from_left_lane, turn(from_left[index], LEFT - RIGHT - STEPS), value)

    pieces = [(which, tile) for which in range(3) for tile in range(tiles)]

    def put(side, x, tile, diff, vel, damp):
        rows = slice(tile * SUB, (tile + 1) * SUB)
        coef[side, 0, x, rows, :] = 1.0 - 6.0 * diff - damp
        coef[side, 1, x, rows, :] = diff
        coef[side, 2, x, rows, :] = vel
        coef[side, 3, x, rows, :] = jnp.where(diff > 0.0, 1.0 / jnp.where(diff > 0.0, diff, 1.0), 0.0)

    def prepare(x, carry):
        for system in range(2):
            for rim in range(rims):
                amp[system, x, rim * SUB : (rim + 1) * SUB, :] = whole_rim((system * rims + rim) * extent + x)
        parts = {}
        for at in range(0, len(pieces), PER):
            packed = whole_rim((2 * rims + at // PER) * extent + x)
            for slot, piece in enumerate(pieces[at : at + PER]):
                alone = turn(jnp.where(lanes // SLOT == slot, packed, 0.0), -slot * SLOT)
                step = SLOT
                while step < LANES:
                    alone = alone + turn(alone, step)
                    step *= 2
                parts[piece] = alone
        for tile in range(tiles):
            rows = slice(tile * SUB, (tile + 1) * SUB)
            put(0, x, tile, *(cell_ref[which, x, rows, :] for which in range(3)))
            put(1, x, tile, *(parts[(which, tile)] for which in range(3)))
        return carry

    lax.fori_loop(0, extent, prepare, 0)

    def spread(side, which, x, y):
        return coef[side, which, x, pl.ds(y, SUB, stride=0), :]

    pad = 2

    def march(system, group, side, load_amp, levels_at):
        low0 = bounds_ref[system, group, 0]
        high0 = bounds_ref[system, group, 1]
        zero = jnp.zeros((SUB, LANES), jnp.float32)

        def blank(target, margin, low, high):
            for x in range(margin, extent - margin):
                for offset in (1, 2):
                    target[x, low - offset + pad] = zero
                    target[x, high + offset + pad] = zero

        heights = levels_at

        def begin(y, carry):
            here = heights == y
            for x in range(extent):
                value = jnp.where(here, load_amp(x), 0.0)
                if system:
                    value = value * spread(side, 1, x, y)
                ping[x, y + pad] = value
            return carry

        lax.fori_loop(low0, high0 + 1, begin, 0)
        blank(ping, 0, low0, high0)
        for level in range(1, STEPS + 1):
            source, target = (ping, pong) if level % 2 else (pong, ping)
            low = jnp.maximum(low0 - level, 0)
            high = jnp.minimum(high0 + level, depth_y - 1)

            def step(y, carry, level=level, source=source, target=target):
                rows = {}
                carried = {}
                for x in range(level - 1, extent - level + 1):
                    rows[x] = source[x, y + pad]
                    if system:
                        carried[x] = rows[x] * spread(side, 2, x, y)
                for x in range(level, extent - level):
                    here = rows[x]
                    behind, ahead = rows[x - 1], rows[x + 1]
                    beside = (source[x, y + pad - 1] + source[x, y + pad + 1]) + (turn(here, 1) + turn(here, -1))
                    if system:
                        drift = carried[x + 1] - carried[x - 1]
                    else:
                        drift = spread(side, 2, x, y) * (behind - ahead)
                    total = beside + (behind + ahead) + drift
                    if system and level == STEPS:
                        value = spread(side, 0, x, y) * (here * spread(side, 3, x, y)) + total
                    else:
                        value = spread(side, 0, x, y) * here + spread(side, 1, x, y) * total
                    if level == STEPS:
                        field[system, x - level, y, group] = value
                    else:
                        target[x, y + pad] = value
                return carry

            lax.fori_loop(low, high + 1, step, 0)
            if level < STEPS:
                blank(target, level, low, high)
            else:

                def clear(y, carry):
                    for x in range(width_x):
                        field[system, x, y, group] = zero
                    return carry

                lax.fori_loop(0, low, clear, 0)
                lax.fori_loop(high + 1, depth_y, clear, 0)

    def main_group(group, carry):
        at = pl.multiple_of(group * SUB, SUB)
        for system in range(2):
            march(
                system, group, 0,
                lambda x, system=system: sorted_ref[system, x, pl.ds(at, SUB), :],
                level_ref[system, pl.ds(at, SUB), :],
            )
        return carry

    lax.fori_loop(0, groups, main_group, 0)

    def rim_group(rim, carry):
        at = pl.multiple_of(rim * SUB, SUB)
        for system in range(2):
            march(
                system, groups + rim, 1,
                lambda x, system=system: amp[system, x, pl.ds(at, SUB), :],
                level_ref[system, pl.ds(inputs + at, SUB), :],
            )
        return carry

    lax.fori_loop(0, rims, rim_group, 0)

    total_ref[...] = jnp.zeros_like(total_ref)
    pairs = depth_y // 2

    def fold(pair, carry):
        x = pair // pairs
        y = (pair % pairs) * 2
        stacked = []
        for system in range(2):
            halves = []
            for half in range(2):
                merged = []
                for group in range(groups):
                    edge = field[system, x, y + half, groups + group // PER]
                    slot = group % PER
                    value = field[system, x, y + half, group]
                    low = turn(edge, -(slot * SLOT + LEFT + STEPS))
                    high = turn(edge, LANES - STEPS - (slot * SLOT + RIGHT + STEPS))
                    value = jnp.where(lanes < STEPS, low, jnp.where(lanes >= LANES - STEPS, high, value))
                    merged.append(value)
                halves.append(jnp.concatenate(merged, axis=0))
            whole = jnp.concatenate(halves, axis=1)
            first, second, third = split(whole)
            out = adjoint_ref if system else direct_ref
            out[pair, 0:inputs, :] = first
            out[pair, inputs : 2 * inputs, :] = second
            stacked.append(jnp.concatenate([first, second, third], axis=0))
        total_ref[...] += lax.dot_general(
            stacked[1], stacked[0], (((1,), (1,)), ((), ())), preferred_element_type=jnp.float32
        )
        return carry

    lax.fori_loop(0, width_x * pairs, fold, 0)

    def part(row, column):
        return total_ref[row * inputs : (row + 1) * inputs, column * inputs : (column + 1) * inputs]

    gram_ref[...] = (
        (part(0, 2) + part(2, 0)) + part(1, 1) + (part(0, 1) + part(1, 0)) + part(0, 0)
    )


def eliminate(matrix):
    size = matrix.shape[0]
    row_ids = lax.broadcasted_iota(jnp.int32, (size, 2 * size), 0)
    column_ids = lax.broadcasted_iota(jnp.int32, (size, 2 * size), 1)
    unit = jnp.where(column_ids - size == row_ids, 1.0, 0.0)
    work = jnp.where(column_ids < size, jnp.concatenate([matrix, matrix], axis=1), unit)
    pivots = jnp.ones((size, 1), jnp.float32)
    ids = lax.broadcasted_iota(jnp.int32, (size, 1), 0)
    for k in range(size):
        row = work[k : k + 1, :]
        pivot = work[k : k + 1, k : k + 1]
        pivots = jnp.where(ids == k, pivot, pivots)
        factor = jnp.where(ids > k, work[:, k : k + 1] / pivot, 0.0)
        work = work - factor * row
    return work[:, size:], pivots


def product(left, right, contract):
    return lax.dot_general(
        left, right, (contract, ((), ())), precision=HIGH, preferred_element_type=jnp.float32
    )


def modes_kernel(
    inputs, width_x, depth_y, scale, rank_ref,
    gram_ref, start_ref, direct_ref, adjoint_ref,
    direct_out, adjoint_out,
    start_sorted,
):
    modes = start_ref.shape[1]

    def move(j, carry):
        start_sorted[pl.ds(rank_ref[0, j], 1), :] = start_ref[pl.ds(j, 1), :]
        return carry

    lax.fori_loop(0, inputs, move, 0, unroll=8)
    gram = gram_ref[...] * scale

    def orthonormal(block):
        lower, pivots = eliminate(product(block, block, ((0,), (0,))))
        return product(block, lower * lax.rsqrt(pivots), ((1,), (1,)))

    first = orthonormal(product(gram, start_sorted[...], ((1,), (0,))))
    right = orthonormal(product(gram, first, ((0,), (0,))))
    reached = product(gram, right, ((1,), (0,)))
    lower, pivots = eliminate(product(reached, reached, ((0,), (0,))))
    root = jnp.sqrt(pivots)
    quarter = jnp.sqrt(root)
    mixes = (
        product(lower / quarter, right, ((1,), (1,))),
        product(lower / (root * quarter), reached, ((1,), (1,))),
    )
    pairs = depth_y // 2
    for mix, source, out in zip(mixes, (direct_ref, adjoint_ref), (direct_out, adjoint_out)):
        high, low, rest = split(mix)
        stacked = jnp.concatenate(
            [jnp.concatenate([high, high], axis=1), jnp.concatenate([low, low], axis=1)], axis=0
        )

        def project(pair, carry, stacked=stacked, source=source, out=out):
            both = jnp.dot(stacked, source[pair], preferred_element_type=jnp.float32)
            value = both[:modes] + both[modes:]
            for half in range(2):
                out[pl.ds(pair * 2 + half, modes, stride=width_x * depth_y), :] = value[
                    :, half * LANES : (half + 1) * LANES
                ]
            return carry

        lax.fori_loop(0, width_x * pairs, project, 0, unroll=4)


def ordering(height):
    count = height.shape[0]
    at = lax.iota(jnp.int32, count)
    ahead = (height[None, :] < height[:, None]) | (
        (height[None, :] == height[:, None]) & (at[None, :] < at[:, None])
    )
    rank = jnp.sum(ahead.astype(jnp.int32), axis=1)
    ordered = jnp.sum(jnp.where(rank[None, :] == at[:, None], height[None, :], 0), axis=1)
    return rank, ordered


def on_device(
    diffusivity,
    velocity,
    damping,
    input_amplitude,
    output_amplitude,
    input_height,
    output_height,
    start_block,
):
    inputs, width_x, width_z = input_amplitude.shape
    depth_y = diffusivity.shape[1]
    rank_count = start_block.shape[1]
    wide = lax.axis_size("wide")
    narrow = lax.axis_size("narrow")
    assert width_z == LANES and width_x == STEPS and inputs % (SUB * PER) == 0
    f32 = jnp.float32
    extent = 3 * width_x
    groups = inputs // SUB
    rims = groups // PER
    tiles = depth_y // SUB

    flat_in = input_amplitude.reshape(-1, width_z)
    flat_out = output_amplitude.reshape(-1, width_z)
    sent = jnp.concatenate(
        [flat_in, flat_out]
        + [cell.reshape(-1, width_z) for cell in (diffusivity, velocity, damping)]
    )
    near_pairs, far_pairs = swaps(wide)
    near = lax.ppermute(sent, "wide", near_pairs)
    far = lax.ppermute(sent, "wide", far_pairs)

    orders = [ordering(height) for height in (input_height, output_height)]
    ranks = jnp.stack([rank for rank, ordered in orders])
    heights = jnp.stack([ordered for rank, ordered in orders])
    by_group = heights.reshape(2, groups, SUB)
    by_rim = heights.reshape(2, rims, PER * SUB)
    bounds = jnp.concatenate(
        [
            jnp.stack([by_group[:, :, 0], by_group[:, :, -1]], axis=-1),
            jnp.stack([by_rim[:, :, 0], by_rim[:, :, -1]], axis=-1),
        ],
        axis=1,
    )
    rim_levels = heights.reshape(2, rims, PER, SUB).transpose(0, 1, 3, 2)
    levels = jnp.concatenate(
        [
            jnp.broadcast_to(heights[:, :, None], (2, inputs, LANES)),
            jnp.repeat(rim_levels, SLOT, axis=-1).reshape(2, rims * SUB, LANES),
        ],
        axis=1,
    )

    odd = lax.axis_index("wide") % 2
    place = jnp.stack([2 * width_x * (1 - odd), 2 * width_x * odd])
    rim_count = (2 * rims + -(-3 * tiles // PER)) * extent
    arranged, cells, rim = pl.pallas_call(
        functools.partial(pack_kernel, inputs, width_x, depth_y),
        out_shape=(
            jax.ShapeDtypeStruct((2, extent, inputs, LANES), f32),
            jax.ShapeDtypeStruct((3, extent, depth_y, LANES), f32),
            jax.ShapeDtypeStruct((rim_count, SUB, LANES), f32),
        ),
        in_specs=[SMEM, SMEM] + [VMEM] * 7,
        out_specs=(VMEM, VMEM, VMEM),
        name="pack",
    )(place, ranks, flat_in, flat_out, diffusivity, velocity, damping, near, far)

    if narrow == 2:
        from_right = lax.ppermute(rim, "narrow", [(0, 1), (1, 0)])
        from_left = from_right
    else:
        from_right = lax.ppermute(rim, "narrow", [(i + 1, i) for i in range(narrow - 1)])
        from_left = lax.ppermute(rim, "narrow", [(i, i + 1) for i in range(narrow - 1)])
    side = lax.axis_index("narrow")
    flags = jnp.stack([(side + 1 < narrow).astype(jnp.int32), (side > 0).astype(jnp.int32)])

    pair_count = width_x * depth_y // 2
    direct, adjoint, gram = pl.pallas_call(
        functools.partial(window_kernel, inputs, width_x, depth_y),
        out_shape=(
            jax.ShapeDtypeStruct((pair_count, 2 * inputs, 2 * LANES), jnp.bfloat16),
            jax.ShapeDtypeStruct((pair_count, 2 * inputs, 2 * LANES), jnp.bfloat16),
            jax.ShapeDtypeStruct((inputs, inputs), f32),
        ),
        in_specs=[SMEM, SMEM] + [VMEM] * 6,
        out_specs=(VMEM, VMEM, VMEM),
        scratch_shapes=[
            pltpu.VMEM((2, extent, rims * SUB, LANES), f32),
            pltpu.VMEM((2, 4, extent, depth_y, LANES), f32),
            pltpu.VMEM((extent, depth_y + 4, SUB, LANES), f32),
            pltpu.VMEM((extent, depth_y + 4, SUB, LANES), f32),
            pltpu.VMEM((2, width_x, depth_y, groups + rims, SUB, LANES), f32),
            pltpu.VMEM((3 * inputs, 3 * inputs), f32),
        ],
        name="window",
    )(bounds, flags, arranged, cells, rim, from_right, from_left, levels)

    step = 1
    while step < wide:
        gram = gram + lax.ppermute(gram, "wide", [(i, i ^ step) for i in range(wide)])
        step *= 2
    step = 1
    while step < narrow:
        gram = gram + lax.ppermute(gram, "narrow", [(i, i ^ step) for i in range(narrow)])
        step *= 2

    scale = 1.0 / math.sqrt(width_x * wide * depth_y * width_z * narrow)
    shape = jax.ShapeDtypeStruct((rank_count * width_x * depth_y, LANES), f32)
    direct_modes, adjoint_modes = pl.pallas_call(
        functools.partial(modes_kernel, inputs, width_x, depth_y, scale),
        out_shape=(shape, shape),
        in_specs=[SMEM] + [VMEM] * 4,
        out_specs=(VMEM, VMEM),
        scratch_shapes=[pltpu.VMEM((inputs, rank_count), f32)],
        name="modes",
    )(ranks, gram, start_block, direct, adjoint)
    full = (rank_count, width_x, depth_y, width_z)
    return (direct_modes.reshape(full), adjoint_modes.reshape(full))


def solution(mesh):
    in_specs = (
        P("wide", None, "narrow"),
        P("wide", None, "narrow"),
        P("wide", None, "narrow"),
        P(None, "wide", "narrow"),
        P(None, "wide", "narrow"),
        P(),
        P(),
        P(),
    )
    out_specs = (P(None, "wide", None, "narrow"), P(None, "wide", None, "narrow"))
    return jax.shard_map(
        on_device, mesh=mesh, in_specs=in_specs, out_specs=out_specs, check_vma=False
    )
```

```python
import functools
import math

import jax
import jax.numpy as jnp
from jax import lax
from jax.experimental import pallas as pl
from jax.experimental.pallas import tpu as pltpu
from jax.sharding import PartitionSpec as P

STEPS = 4
HIGH = lax.Precision.HIGHEST
LANES = 128
SUB = 8
SLOT = 32
PER = LANES // SLOT
LEFT = 0
RIGHT = 16
REACH = STEPS + SUB

VMEM = pl.BlockSpec(memory_space=pltpu.VMEM)
SMEM = pl.BlockSpec(memory_space=pltpu.SMEM)


def swaps(count):
    near = [(i, i ^ 1) for i in range(count) if i ^ 1 < count]
    far = [(i, ((i + 1) ^ 1) - 1) for i in range(count) if 0 <= ((i + 1) ^ 1) - 1 < count]
    return near, far


def lane_ids(shape):
    return lax.broadcasted_iota(jnp.int32, shape, len(shape) - 1)


def turn(value, amount):
    return pltpu.roll(value, amount % LANES, value.ndim - 1)


def edges(block, slot):
    within = lane_ids(block.shape) - slot * SLOT
    low = turn(block, slot * SLOT + LEFT + STEPS)
    high = turn(block, slot * SLOT + RIGHT - (LANES - SUB))
    is_low = (within >= LEFT + STEPS) & (within < LEFT + REACH)
    is_high = (within >= RIGHT) & (within < RIGHT + SUB)
    return jnp.where(is_low, low, jnp.where(is_high, high, 0.0))


def stage_kernel(*refs):
    sources, target, sems = refs[:-2], refs[-2], refs[-1]
    copies = []
    at = 0
    for index, source in enumerate(sources):
        count = source.shape[0]
        copies.append(pltpu.make_async_copy(source, target.at[pl.ds(at, count)], sems.at[index]))
        at += count
    for copy in copies:
        copy.start()
    for copy in copies:
        copy.wait()


def pack_kernel(
    inputs, width_x, depth_y, place_ref, rank_ref, here, near, far,
    sorted_ref, cell_ref, rim_ref,
):
    own = width_x
    near_x = place_ref[0]
    far_x = place_ref[1]
    for system in range(2):
        base = system * inputs * width_x

        def move(j, carry, system=system, base=base):
            to = rank_ref[system, j]
            for x in range(width_x):
                row = base + j * width_x + x
                sorted_ref[system, own + x, pl.ds(to, 1), :] = here[pl.ds(row, 1), :]
                sorted_ref[system, near_x + x, pl.ds(to, 1), :] = near[pl.ds(row, 1), :]
                sorted_ref[system, far_x + x, pl.ds(to, 1), :] = far[pl.ds(row, 1), :]
            return carry

        lax.fori_loop(0, inputs, move, 0, unroll=4)
    start = 2 * inputs * width_x
    for which in range(3):
        for x in range(width_x):
            rows = pl.ds(start + (which * width_x + x) * depth_y, depth_y)
            cell_ref[which, own + x] = here[rows, :]
            cell_ref[which, near_x + x] = near[rows, :]
            cell_ref[which, far_x + x] = far[rows, :]
    groups = inputs // SUB
    rims = groups // PER
    extent = 3 * width_x
    tiles = depth_y // SUB

    def rim_row(x, carry):
        for system in range(2):
            for rim in range(rims):
                total = jnp.zeros((SUB, LANES), jnp.float32)
                for slot in range(PER):
                    group = rim * PER + slot
                    total = total + edges(sorted_ref[system, x, group * SUB : (group + 1) * SUB, :], slot)
                rim_ref[(system * rims + rim) * extent + x] = total
        pieces = [(which, tile) for which in range(3) for tile in range(tiles)]
        for at in range(0, len(pieces), PER):
            total = jnp.zeros((SUB, LANES), jnp.float32)
            for slot, (which, tile) in enumerate(pieces[at : at + PER]):
                total = total + edges(cell_ref[which, x, tile * SUB : (tile + 1) * SUB, :], slot)
            rim_ref[(2 * rims + at // PER) * extent + x] = total
        return carry

    lax.fori_loop(0, extent, rim_row, 0, unroll=extent)


def split(value):
    first = value.astype(jnp.bfloat16)
    rest = value - first.astype(jnp.float32)
    second = rest.astype(jnp.bfloat16)
    third = (rest - second.astype(jnp.float32)).astype(jnp.bfloat16)
    return first, second, third


def window_kernel(
    inputs, width_x, depth_y, bounds_ref, flag_ref,
    sorted_ref, cell_ref, rim_ref, from_right, from_left, level_ref,
    direct_ref, adjoint_ref, gram_ref,
    amp, coef, ping, pong, field, total_ref,
):
    groups = inputs // SUB
    rims = groups // PER
    extent = 3 * width_x
    tiles = depth_y // SUB
    lanes = lane_ids((SUB, LANES))
    within = lanes % SLOT
    from_right_lane = (within >= RIGHT + SUB) & (within < RIGHT + REACH) & (flag_ref[0] > 0)
    from_left_lane = (within >= LEFT) & (within < LEFT + STEPS) & (flag_ref[1] > 0)

    def whole_rim(index):
        value = rim_ref[index]
        value = jnp.where(from_right_lane, turn(from_right[index], RIGHT + SUB - STEPS), value)
        return jnp.where(from_left_lane, turn(from_left[index], LEFT - RIGHT - STEPS), value)

    pieces = [(which, tile) for which in range(3) for tile in range(tiles)]

    def put(side, x, tile, diff, vel, damp):
        inverse = jnp.where(diff > 0.0, 1.0 / jnp.where(diff > 0.0, diff, 1.0), 0.0)
        for which, value in enumerate((1.0 - 6.0 * diff - damp, diff, vel, inverse)):
            for y in range(SUB):
                coef[side, which, x, tile * SUB + y] = jnp.broadcast_to(value[y : y + 1, :], (SUB, LANES))

    def prepare(x, carry):
        for system in range(2):
            for rim in range(rims):
                amp[system, x, rim * SUB : (rim + 1) * SUB, :] = whole_rim((system * rims + rim) * extent + x)
        parts = {}
        for at in range(0, len(pieces), PER):
            packed = whole_rim((2 * rims + at // PER) * extent + x)
            for slot, piece in enumerate(pieces[at : at + PER]):
                alone = turn(jnp.where(lanes // SLOT == slot, packed, 0.0), -slot * SLOT)
                step = SLOT
                while step < LANES:
                    alone = alone + turn(alone, step)
                    step *= 2
                parts[piece] = alone
        for tile in range(tiles):
            rows = slice(tile * SUB, (tile + 1) * SUB)
            put(0, x, tile, *(cell_ref[which, x, rows, :] for which in range(3)))
            put(1, x, tile, *(parts[(which, tile)] for which in range(3)))
        return carry

    lax.fori_loop(0, extent, prepare, 0, unroll=extent)

    def spread(side, which, x, y):
        return coef[side, which, x, y]

    pad = 2
    zero = jnp.zeros((SUB, LANES), jnp.float32)

    def march(system):
        units = range(groups + rims)
        side = [int(unit >= groups) for unit in units]
        low0 = [bounds_ref[system, unit, 0] for unit in units]
        high0 = [bounds_ref[system, unit, 1] for unit in units]

        def blank(target, unit, margin, low, high):
            for x in range(margin, extent - margin):
                for offset in (1, 2):
                    target[unit, x, low - offset + pad] = zero
                    target[unit, x, high + offset + pad] = zero

        for unit in units:
            rows = slice(unit * SUB, (unit + 1) * SUB)
            heights = level_ref[system, rows, :]

            def begin(y, carry, unit=unit, rows=rows, heights=heights):
                here = heights == y
                for x in range(extent):
                    if side[unit]:
                        value = amp[system, x, (unit - groups) * SUB : (unit - groups + 1) * SUB, :]
                    else:
                        value = sorted_ref[system, x, rows, :]
                    value = jnp.where(here, value, 0.0)
                    if system:
                        value = value * spread(side[unit], 1, x, y)
                    ping[unit, x, y + pad] = value
                return carry

            lax.fori_loop(low0[unit], high0[unit] + 1, begin, 0)
            blank(ping, unit, 0, low0[unit], high0[unit])

        for level in range(1, STEPS + 1):
            source, target = (ping, pong) if level % 2 else (pong, ping)
            low = [jnp.maximum(bound - level, 0) for bound in low0]
            high = [jnp.minimum(bound + level, depth_y - 1) for bound in high0]
            trips = functools.reduce(
                jnp.maximum,
                [(high[unit] - low[unit] + 1 + side[unit]) // (1 + side[unit]) for unit in units],
            )

            def plane(unit, y, level=level, source=source, target=target):
                rows = {}
                carried = {}
                for x in range(level - 1, extent - level + 1):
                    rows[x] = source[unit, x, y + pad]
                    if system:
                        carried[x] = rows[x] * spread(side[unit], 2, x, y)
                for x in range(level, extent - level):
                    here = rows[x]
                    behind, ahead = rows[x - 1], rows[x + 1]
                    beside = (source[unit, x, y + pad - 1] + source[unit, x, y + pad + 1]) + (
                        turn(here, 1) + turn(here, -1)
                    )
                    if system:
                        drift = carried[x + 1] - carried[x - 1]
                    else:
                        drift = spread(side[unit], 2, x, y) * (behind - ahead)
                    total = beside + (behind + ahead) + drift
                    if system and level == STEPS:
                        value = spread(side[unit], 0, x, y) * (here * spread(side[unit], 3, x, y)) + total
                    else:
                        value = spread(side[unit], 0, x, y) * here + spread(side[unit], 1, x, y) * total
                    if level == STEPS:
                        field[system, x - level, y, unit] = value
                    else:
                        target[unit, x, y + pad] = value

            def step(trip, carry, low=low, high=high, plane=plane):
                for unit in units:
                    span = 1 + side[unit]
                    for more in range(span):
                        plane(unit, jnp.minimum(low[unit] + (trip * span + more), high[unit]))
                return carry

            lax.fori_loop(0, trips, step, 0)
            for unit in units:
                if level < STEPS:
                    blank(target, unit, level, low[unit], high[unit])
                else:

                    def clear(y, carry, unit=unit):
                        for x in range(width_x):
                            field[system, x, y, unit] = zero
                        return carry

                    lax.fori_loop(0, low[unit], clear, 0)
                    lax.fori_loop(high[unit] + 1, depth_y, clear, 0)

    for system in range(2):
        march(system)

    total_ref[...] = jnp.zeros_like(total_ref)
    pairs = depth_y // 2

    def fold(pair, carry):
        x = pair // pairs
        y = (pair % pairs) * 2
        stacked = []
        for system in range(2):
            halves = []
            for half in range(2):
                merged = []
                for group in range(groups):
                    edge = field[system, x, y + half, groups + group // PER]
                    slot = group % PER
                    value = field[system, x, y + half, group]
                    low = turn(edge, -(slot * SLOT + LEFT + STEPS))
                    high = turn(edge, LANES - STEPS - (slot * SLOT + RIGHT + STEPS))
                    value = jnp.where(lanes < STEPS, low, jnp.where(lanes >= LANES - STEPS, high, value))
                    merged.append(value)
                halves.append(jnp.concatenate(merged, axis=0))
            whole = jnp.concatenate(halves, axis=1)
            first, second, third = split(whole)
            out = adjoint_ref if system else direct_ref
            out[pair, 0:inputs, :] = first
            out[pair, inputs : 2 * inputs, :] = second
            stacked.append(jnp.concatenate([first, second, third], axis=0))
        total_ref[...] += lax.dot_general(
            stacked[1], stacked[0], (((1,), (1,)), ((), ())), preferred_element_type=jnp.float32
        )
        return carry

    lax.fori_loop(0, width_x * pairs, fold, 0, unroll=4)

    def part(row, column):
        return total_ref[row * inputs : (row + 1) * inputs, column * inputs : (column + 1) * inputs]

    gram_ref[...] = (
        (part(0, 2) + part(2, 0)) + part(1, 1) + (part(0, 1) + part(1, 0)) + part(0, 0)
    )


def eliminate(matrix):
    size = matrix.shape[0]
    tiles = size // SUB
    row_ids = lax.broadcasted_iota(jnp.int32, (SUB, LANES), 0)
    columns = {}
    for j in range(size):
        for tile in range(j // SUB, tiles):
            part = matrix[tile * SUB : (tile + 1) * SUB, j : j + 1]
            columns[j, tile] = jnp.broadcast_to(part, (SUB, LANES))
    lanes = lane_ids((SUB, LANES))
    inverse = [jnp.where(lanes - tile * SUB == row_ids, 1.0, 0.0) for tile in range(tiles)]
    pivots = [jnp.ones((SUB, LANES), jnp.float32) for tile in range(tiles)]

    def pick(tile, row):
        return jnp.broadcast_to(tile[row : row + 1, :], (SUB, LANES))

    for k in range(size):
        home, place = k // SUB, k % SUB
        pivot = pick(columns[k, home], place)
        pivots[home] = jnp.where(row_ids == place, pivot, pivots[home])
        reciprocal = 1.0 / pivot
        factors = {}
        for tile in range(home, tiles):
            factors[tile] = columns[k, tile] * reciprocal
        factors[home] = jnp.where(row_ids > place, factors[home], 0.0)
        for j in range(k + 1, size):
            across = pick(columns[k, j // SUB], j % SUB)
            for tile in range(j // SUB, tiles):
                columns[j, tile] = columns[j, tile] - factors[tile] * across
        source = pick(inverse[home], place)
        for tile in range(home, tiles):
            inverse[tile] = inverse[tile] - factors[tile] * source
    lower = jnp.concatenate(inverse, axis=0)[:, :size]
    return lower, jnp.concatenate(pivots, axis=0)[:, :size]


def product(left, right, contract):
    return lax.dot_general(
        left, right, (contract, ((), ())), precision=HIGH, preferred_element_type=jnp.float32
    )


def modes_kernel(
    inputs, width_x, depth_y, scale, rank_ref,
    gram_ref, start_ref, direct_ref, adjoint_ref,
    direct_out, adjoint_out,
    start_sorted,
):
    modes = start_ref.shape[1]

    def move(j, carry):
        start_sorted[pl.ds(rank_ref[0, j], 1), :] = start_ref[pl.ds(j, 1), :]
        return carry

    lax.fori_loop(0, inputs, move, 0, unroll=8)
    gram = gram_ref[...] * scale

    def orthonormal(block):
        lower, pivots = eliminate(product(block, block, ((0,), (0,))))
        return product(block, lower * lax.rsqrt(pivots), ((1,), (1,)))

    first = orthonormal(product(gram, start_sorted[...], ((1,), (0,))))
    right = orthonormal(product(gram, first, ((0,), (0,))))
    reached = product(gram, right, ((1,), (0,)))
    lower, pivots = eliminate(product(reached, reached, ((0,), (0,))))
    root = jnp.sqrt(pivots)
    quarter = jnp.sqrt(root)
    mixes = (
        product(lower / quarter, right, ((1,), (1,))),
        product(lower / (root * quarter), reached, ((1,), (1,))),
    )
    pairs = depth_y // 2
    for mix, source, out in zip(mixes, (direct_ref, adjoint_ref), (direct_out, adjoint_out)):
        high, low, rest = split(mix)
        stacked = jnp.concatenate(
            [jnp.concatenate([high, high], axis=1), jnp.concatenate([low, low], axis=1)], axis=0
        )

        def project(pair, carry, stacked=stacked, source=source, out=out):
            both = jnp.dot(stacked, source[pair], preferred_element_type=jnp.float32)
            value = both[:modes] + both[modes:]
            for half in range(2):
                out[pl.ds(pair * 2 + half, modes, stride=width_x * depth_y), :] = value[
                    :, half * LANES : (half + 1) * LANES
                ]
            return carry

        lax.fori_loop(0, width_x * pairs, project, 0, unroll=8)


def ordering(height):
    count = height.shape[0]
    at = lax.iota(jnp.int32, count)
    ahead = (height[None, :] < height[:, None]) | (
        (height[None, :] == height[:, None]) & (at[None, :] < at[:, None])
    )
    rank = jnp.sum(ahead.astype(jnp.int32), axis=1)
    ordered = jnp.sum(jnp.where(rank[None, :] == at[:, None], height[None, :], 0), axis=1)
    return rank, ordered


def everywhere(value, wide, narrow):
    axes = ("wide", "narrow")
    count = wide * narrow
    if count & (count - 1):
        return lax.psum(value, axes)
    bits = [narrow << i for i in range(wide.bit_length() - 1)]
    bits += [1 << i for i in range(narrow.bit_length() - 1)]

    def other(value, bit):
        return lax.ppermute(value, axes, [(i, i ^ bit) for i in range(count)])

    if bits:
        value = value + other(value, bits[0])
    rest = bits[1:]
    for at in range(0, len(rest), 2):
        pair = rest[at : at + 2]
        if len(pair) == 1:
            value = value + other(value, pair[0])
        else:
            first, second = pair
            value = (value + other(value, first)) + (other(value, second) + other(value, first ^ second))
    return value


def on_device(
    diffusivity,
    velocity,
    damping,
    input_amplitude,
    output_amplitude,
    input_height,
    output_height,
    start_block,
):
    inputs, width_x, width_z = input_amplitude.shape
    depth_y = diffusivity.shape[1]
    rank_count = start_block.shape[1]
    wide = lax.axis_size("wide")
    narrow = lax.axis_size("narrow")
    assert width_z == LANES and width_x == STEPS and inputs % (SUB * PER) == 0
    f32 = jnp.float32
    extent = 3 * width_x
    groups = inputs // SUB
    rims = groups // PER
    tiles = depth_y // SUB

    flat_in = input_amplitude.reshape(-1, width_z)
    flat_out = output_amplitude.reshape(-1, width_z)
    pieces = [flat_in, flat_out] + [
        cell.reshape(-1, width_z) for cell in (diffusivity, velocity, damping)
    ]
    sent = pl.pallas_call(
        stage_kernel,
        out_shape=jax.ShapeDtypeStruct((sum(piece.shape[0] for piece in pieces), width_z), f32),
        in_specs=[pl.BlockSpec(memory_space=pltpu.HBM)] * len(pieces),
        out_specs=VMEM,
        scratch_shapes=[pltpu.SemaphoreType.DMA((len(pieces),))],
        compiler_params=pltpu.CompilerParams(vmem_limit_bytes=60 * 1024 * 1024),
        name="stage",
    )(*pieces)
    near_pairs, far_pairs = swaps(wide)
    near = lax.ppermute(sent, "wide", near_pairs)
    far = lax.ppermute(sent, "wide", far_pairs)

    orders = [ordering(height) for height in (input_height, output_height)]
    ranks = jnp.stack([rank for rank, ordered in orders])
    heights = jnp.stack([ordered for rank, ordered in orders])
    by_group = heights.reshape(2, groups, SUB)
    by_rim = heights.reshape(2, rims, PER * SUB)
    bounds = jnp.concatenate(
        [
            jnp.stack([by_group[:, :, 0], by_group[:, :, -1]], axis=-1),
            jnp.stack([by_rim[:, :, 0], by_rim[:, :, -1]], axis=-1),
        ],
        axis=1,
    )
    rim_levels = heights.reshape(2, rims, PER, SUB).transpose(0, 1, 3, 2)
    levels = jnp.concatenate(
        [
            jnp.broadcast_to(heights[:, :, None], (2, inputs, LANES)),
            jnp.repeat(rim_levels, SLOT, axis=-1).reshape(2, rims * SUB, LANES),
        ],
        axis=1,
    )

    odd = lax.axis_index("wide") % 2
    place = jnp.stack([2 * width_x * (1 - odd), 2 * width_x * odd])
    rim_count = (2 * rims + -(-3 * tiles // PER)) * extent
    arranged, cells, rim = pl.pallas_call(
        functools.partial(pack_kernel, inputs, width_x, depth_y),
        out_shape=(
            jax.ShapeDtypeStruct((2, extent, inputs, LANES), f32),
            jax.ShapeDtypeStruct((3, extent, depth_y, LANES), f32),
            jax.ShapeDtypeStruct((rim_count, SUB, LANES), f32),
        ),
        in_specs=[SMEM, SMEM] + [VMEM] * 3,
        out_specs=(VMEM, VMEM, VMEM),
        compiler_params=pltpu.CompilerParams(vmem_limit_bytes=8 << 20),
        name="pack",
    )(place, ranks, sent, near, far)

    if narrow == 2:
        from_right = lax.ppermute(rim, "narrow", [(0, 1), (1, 0)])
        from_left = from_right
    else:
        from_right = lax.ppermute(rim, "narrow", [(i + 1, i) for i in range(narrow - 1)])
        from_left = lax.ppermute(rim, "narrow", [(i, i + 1) for i in range(narrow - 1)])
    side = lax.axis_index("narrow")
    flags = jnp.stack([(side + 1 < narrow).astype(jnp.int32), (side > 0).astype(jnp.int32)])

    pair_count = width_x * depth_y // 2
    direct, adjoint, gram = pl.pallas_call(
        functools.partial(window_kernel, inputs, width_x, depth_y),
        out_shape=(
            jax.ShapeDtypeStruct((pair_count, 2 * inputs, 2 * LANES), jnp.bfloat16),
            jax.ShapeDtypeStruct((pair_count, 2 * inputs, 2 * LANES), jnp.bfloat16),
            jax.ShapeDtypeStruct((inputs, inputs), f32),
        ),
        in_specs=[SMEM, SMEM] + [VMEM] * 6,
        out_specs=(VMEM, VMEM, VMEM),
        scratch_shapes=[
            pltpu.VMEM((2, extent, rims * SUB, LANES), f32),
            pltpu.VMEM((2, 4, extent, depth_y, SUB, LANES), f32),
            pltpu.VMEM((groups + rims, extent, depth_y + 4, SUB, LANES), f32),
            pltpu.VMEM((groups + rims, extent, depth_y + 4, SUB, LANES), f32),
            pltpu.VMEM((2, width_x, depth_y, groups + rims, SUB, LANES), f32),
            pltpu.VMEM((3 * inputs, 3 * inputs), f32),
        ],
        compiler_params=pltpu.CompilerParams(vmem_limit_bytes=34 << 20),
        name="window",
    )(bounds, flags, arranged, cells, rim, from_right, from_left, levels)

    gram = everywhere(gram, wide, narrow)

    scale = 1.0 / math.sqrt(width_x * wide * depth_y * width_z * narrow)
    shape = jax.ShapeDtypeStruct((rank_count * width_x * depth_y, LANES), f32)
    direct_modes, adjoint_modes = pl.pallas_call(
        functools.partial(modes_kernel, inputs, width_x, depth_y, scale),
        out_shape=(shape, shape),
        in_specs=[SMEM] + [VMEM] * 4,
        out_specs=(VMEM, VMEM),
        scratch_shapes=[pltpu.VMEM((inputs, rank_count), f32)],
        compiler_params=pltpu.CompilerParams(vmem_limit_bytes=7 << 20),
        name="modes",
    )(ranks, gram, start_block, direct, adjoint)
    full = (rank_count, width_x, depth_y, width_z)
    return (direct_modes.reshape(full), adjoint_modes.reshape(full))


def solution(mesh):
    in_specs = (
        P("wide", None, "narrow"),
        P("wide", None, "narrow"),
        P("wide", None, "narrow"),
        P(None, "wide", "narrow"),
        P(None, "wide", "narrow"),
        P(),
        P(),
        P(),
    )
    out_specs = (P(None, "wide", None, "narrow"), P(None, "wide", None, "narrow"))
    return jax.shard_map(
        on_device, mesh=mesh, in_specs=in_specs, out_specs=out_specs, check_vma=False
    )
```

```python
import functools
import math

import jax
import jax.numpy as jnp
from jax import lax
from jax.experimental import pallas as pl
from jax.experimental.pallas import tpu as pltpu
from jax.sharding import PartitionSpec as P

STEPS = 4
HIGH = lax.Precision.HIGHEST
LANES = 128
SUB = 8
SLOT = 32
PER = LANES // SLOT
LEFT = 0
RIGHT = 16
REACH = STEPS + SUB
PAD = STEPS + 1

VMEM = pl.BlockSpec(memory_space=pltpu.VMEM)
SMEM = pl.BlockSpec(memory_space=pltpu.SMEM)


def swaps(count):
    near = [(i, i ^ 1) for i in range(count) if i ^ 1 < count]
    far = [(i, ((i + 1) ^ 1) - 1) for i in range(count) if 0 <= ((i + 1) ^ 1) - 1 < count]
    return near, far


def lane_ids(shape):
    return lax.broadcasted_iota(jnp.int32, shape, len(shape) - 1)


def turn(value, amount):
    return pltpu.roll(value, amount % LANES, value.ndim - 1)


def edges(block, slot):
    within = lane_ids(block.shape) - slot * SLOT
    low = turn(block, slot * SLOT + LEFT + STEPS)
    high = turn(block, slot * SLOT + RIGHT - (LANES - SUB))
    is_low = (within >= LEFT + STEPS) & (within < LEFT + REACH)
    is_high = (within >= RIGHT) & (within < RIGHT + SUB)
    return jnp.where(is_low, low, jnp.where(is_high, high, 0.0))


def stage_kernel(*refs):
    sources, target, sems = refs[:-2], refs[-2], refs[-1]
    copies = []
    at = 0
    for index, source in enumerate(sources):
        count = source.shape[0]
        copies.append(pltpu.make_async_copy(source, target.at[pl.ds(at, count)], sems.at[index]))
        at += count
    for copy in copies:
        copy.start()
    for copy in copies:
        copy.wait()


def pack_kernel(
    inputs, width_x, depth_y, place_ref, rank_ref, here, near, far,
    sorted_ref, cell_ref, rim_ref,
):
    own = width_x
    near_x = place_ref[0]
    far_x = place_ref[1]
    for system in range(2):
        base = system * inputs * width_x

        def move(j, carry, system=system, base=base):
            to = rank_ref[system, j]
            for x in range(width_x):
                row = base + j * width_x + x
                sorted_ref[system, own + x, pl.ds(to, 1), :] = here[pl.ds(row, 1), :]
                sorted_ref[system, near_x + x, pl.ds(to, 1), :] = near[pl.ds(row, 1), :]
                sorted_ref[system, far_x + x, pl.ds(to, 1), :] = far[pl.ds(row, 1), :]
            return carry

        lax.fori_loop(0, inputs, move, 0, unroll=4)
    start = 2 * inputs * width_x
    for which in range(3):
        for x in range(width_x):
            rows = pl.ds(start + (which * width_x + x) * depth_y, depth_y)
            cell_ref[which, own + x] = here[rows, :]
            cell_ref[which, near_x + x] = near[rows, :]
            cell_ref[which, far_x + x] = far[rows, :]
    groups = inputs // SUB
    rims = groups // PER
    extent = 3 * width_x
    tiles = depth_y // SUB

    def rim_row(x, carry):
        for system in range(2):
            for rim in range(rims):
                total = jnp.zeros((SUB, LANES), jnp.float32)
                for slot in range(PER):
                    group = rim * PER + slot
                    total = total + edges(sorted_ref[system, x, group * SUB : (group + 1) * SUB, :], slot)
                rim_ref[(system * rims + rim) * extent + x] = total
        pieces = [(which, tile) for which in range(3) for tile in range(tiles)]
        for at in range(0, len(pieces), PER):
            total = jnp.zeros((SUB, LANES), jnp.float32)
            for slot, (which, tile) in enumerate(pieces[at : at + PER]):
                total = total + edges(cell_ref[which, x, tile * SUB : (tile + 1) * SUB, :], slot)
            rim_ref[(2 * rims + at // PER) * extent + x] = total
        return carry

    lax.fori_loop(0, extent, rim_row, 0, unroll=extent)


def split(value):
    first = value.astype(jnp.bfloat16)
    rest = value - first.astype(jnp.float32)
    second = rest.astype(jnp.bfloat16)
    third = (rest - second.astype(jnp.float32)).astype(jnp.bfloat16)
    return first, second, third


def store_cells(coef, x, tile, diff, vel, damp):
    inverse = jnp.where(diff > 0.0, 1.0 / jnp.where(diff > 0.0, diff, 1.0), 0.0)
    for which, value in enumerate((1.0 - 6.0 * diff - damp, diff, vel, inverse)):
        for y in range(SUB):
            coef[which, x, tile * SUB + y] = jnp.broadcast_to(value[y : y + 1, :], (SUB, LANES))


def march(units, share, depth_y, extent, bounds, load, heights, coef, ping, pong, write, wipe):
    zero = jnp.zeros((SUB, LANES), jnp.float32)
    count = len(units)
    low0 = [bounds[system, row, 0] for system, row in units]
    high0 = [bounds[system, row, 1] for system, row in units]
    top = depth_y - 1

    for at in range(count):
        levels = heights(at)
        for x in range(extent):
            for buffer in (ping, pong):
                buffer[at, x, PAD - 1] = zero
                buffer[at, x, PAD + depth_y] = zero

        def begin(y, carry, at=at, levels=levels):
            here = levels == y
            for x in range(extent):
                value = jnp.where(here, load(at, x), 0.0)
                if units[at][0]:
                    value = value * coef[1, x, y]
                ping[at, x, y + PAD] = value
            return carry

        lax.fori_loop(low0[at], high0[at] + 1, begin, 0)
        for x in range(1, extent - 1):
            ping[at, x, low0[at] - 1 + PAD] = zero
            ping[at, x, high0[at] + 1 + PAD] = zero

    for level in range(1, STEPS + 1):
        source, target = (ping, pong) if level % 2 else (pong, ping)
        low = [jnp.maximum(bound - level + 1, 0) for bound in low0]
        high = [jnp.minimum(bound + level - 1, top) for bound in high0]
        trips = functools.reduce(
            jnp.maximum, [(high[at] - low[at] + share) // share for at in range(count)]
        )

        def plane(at, y, level=level, source=source, target=target):
            system = units[at][0]
            rows = {}
            carried = {}
            for x in range(level - 1, extent - level + 1):
                rows[x] = source[at, x, y + PAD]
                if system:
                    carried[x] = rows[x] * coef[2, x, y]
            for x in range(level, extent - level):
                here = rows[x]
                behind, ahead = rows[x - 1], rows[x + 1]
                beside = (source[at, x, y + PAD - 1] + source[at, x, y + PAD + 1]) + (
                    turn(here, 1) + turn(here, -1)
                )
                if system:
                    drift = carried[x + 1] - carried[x - 1]
                else:
                    drift = coef[2, x, y] * (behind - ahead)
                total = beside + (behind + ahead) + drift
                if system and level == STEPS:
                    value = coef[0, x, y] * (here * coef[3, x, y]) + total
                else:
                    value = coef[0, x, y] * here + coef[1, x, y] * total
                if level == STEPS:
                    write(at, x - level, y, value)
                else:
                    target[at, x, y + PAD] = value

        def step(trip, carry, low=low, high=high, plane=plane):
            for at in range(count):
                for more in range(share):
                    plane(at, jnp.minimum(low[at] + (trip * share + more), high[at]))
            return carry

        lax.fori_loop(0, trips, step, 0)
        for at in range(count):
            for y, inner, outer in (
                (low0[at] - level, 1, -1),
                (high0[at] + level, -1, 1),
            ):
                inside = (y >= 0) & (y <= top)
                if level < STEPS:
                    near = jnp.minimum(jnp.maximum(y, 0), top)
                    for x in range(level, extent - level):
                        value = coef[1, x, near] * source[at, x, y + inner + PAD]
                        target[at, x, y + PAD] = jnp.where(inside, value, 0.0)
                        if level < x < extent - level - 1:
                            target[at, x, y + outer + PAD] = zero
                else:

                    @pl.when(inside)
                    def _(at=at, y=y, inner=inner, level=level, source=source):
                        for x in range(level, extent - level):
                            value = source[at, x, y + inner + PAD]
                            if not units[at][0]:
                                value = coef[1, x, y] * value
                            write(at, x - level, y, value)

            if level == STEPS:

                def clear(y, carry, at=at):
                    wipe(at, y, zero)
                    return carry

                lax.fori_loop(0, low0[at] - level, clear, 0)
                lax.fori_loop(high0[at] + level + 1, depth_y, clear, 0)


def main_kernel(
    inputs, width_x, depth_y, bounds_ref, sorted_ref, cell_ref, level_ref, field, coef, ping, pong
):
    groups = inputs // SUB
    extent = 3 * width_x

    def prepare(x, carry):
        for tile in range(depth_y // SUB):
            rows = slice(tile * SUB, (tile + 1) * SUB)
            store_cells(coef, x, tile, *(cell_ref[which, x, rows, :] for which in range(3)))
        return carry

    lax.fori_loop(0, extent, prepare, 0, unroll=2)
    units = [(system, group) for system in range(2) for group in range(groups)]

    def rows(at):
        return slice(units[at][1] * SUB, (units[at][1] + 1) * SUB)

    def write(at, x, y, value):
        field[units[at][0], x, y, units[at][1]] = value

    def wipe(at, y, zero):
        for x in range(width_x):
            write(at, x, y, zero)

    march(
        units, 1, depth_y, extent, bounds_ref,
        lambda at, x: sorted_ref[units[at][0], x, rows(at), :],
        lambda at: level_ref[units[at][0], rows(at), :],
        coef, ping, pong, write, wipe,
    )


def rim_kernel(
    inputs, width_x, depth_y, bounds_ref, flag_ref,
    rim_ref, from_right, from_left, level_ref, field,
    direct_ref, adjoint_ref, gram_ref,
    amp, coef, ping, pong, edge_field, total_ref,
):
    groups = inputs // SUB
    rims = groups // PER
    extent = 3 * width_x
    tiles = depth_y // SUB
    lanes = lane_ids((SUB, LANES))
    within = lanes % SLOT
    from_right_lane = (within >= RIGHT + SUB) & (within < RIGHT + REACH) & (flag_ref[0] > 0)
    from_left_lane = (within >= LEFT) & (within < LEFT + STEPS) & (flag_ref[1] > 0)

    def whole_rim(index):
        value = rim_ref[index]
        value = jnp.where(from_right_lane, turn(from_right[index], RIGHT + SUB - STEPS), value)
        return jnp.where(from_left_lane, turn(from_left[index], LEFT - RIGHT - STEPS), value)

    pieces = [(which, tile) for which in range(3) for tile in range(tiles)]

    def prepare(x, carry):
        for system in range(2):
            for rim in range(rims):
                amp[system * rims + rim, x] = whole_rim((system * rims + rim) * extent + x)
        parts = {}
        for at in range(0, len(pieces), PER):
            packed = whole_rim((2 * rims + at // PER) * extent + x)
            for slot, piece in enumerate(pieces[at : at + PER]):
                alone = turn(jnp.where(lanes // SLOT == slot, packed, 0.0), -slot * SLOT)
                step = SLOT
                while step < LANES:
                    alone = alone + turn(alone, step)
                    step *= 2
                parts[piece] = alone
        for tile in range(tiles):
            store_cells(coef, x, tile, *(parts[(which, tile)] for which in range(3)))
        return carry

    lax.fori_loop(0, extent, prepare, 0, unroll=extent)
    units = [(system, groups + rim) for system in range(2) for rim in range(rims)]

    def rows(at):
        return slice(units[at][1] * SUB, (units[at][1] + 1) * SUB)

    def write(at, x, y, value):
        edge_field[at, x, y] = value

    def wipe(at, y, zero):
        for x in range(width_x):
            write(at, x, y, zero)

    march(
        units, 2, depth_y, extent, bounds_ref,
        lambda at, x: amp[at, x],
        lambda at: level_ref[units[at][0], rows(at), :],
        coef, ping, pong, write, wipe,
    )

    total_ref[...] = jnp.zeros_like(total_ref)
    pairs = depth_y // 2

    def fold(pair, carry):
        x = pair // pairs
        y = (pair % pairs) * 2
        stacked = []
        for system in range(2):
            halves = []
            for half in range(2):
                merged = []
                for rim in range(rims):
                    edge = edge_field[system * rims + rim, x, y + half]
                    edge = jnp.where(within < LEFT + STEPS, turn(edge, LEFT - RIGHT - STEPS), edge)
                    for slot in range(PER):
                        value = field[system, x, y + half, rim * PER + slot]
                        both = turn(edge, -(slot * SLOT + LEFT + STEPS))
                        outer = (lanes < STEPS) | (lanes >= LANES - STEPS)
                        merged.append(jnp.where(outer, both, value))
                halves.append(jnp.concatenate(merged, axis=0))
            whole = jnp.concatenate(halves, axis=1)
            first, second, third = split(whole)
            out = adjoint_ref if system else direct_ref
            out[pair, 0:inputs, :] = first
            out[pair, inputs : 2 * inputs, :] = second
            stacked.append(jnp.concatenate([first, second, third], axis=0))
        total_ref[...] += lax.dot_general(
            stacked[1], stacked[0], (((1,), (1,)), ((), ())), preferred_element_type=jnp.float32
        )
        return carry

    lax.fori_loop(0, width_x * pairs, fold, 0, unroll=4)

    def part(row, column):
        return total_ref[row * inputs : (row + 1) * inputs, column * inputs : (column + 1) * inputs]

    gram_ref[...] = (
        (part(0, 2) + part(2, 0)) + part(1, 1) + (part(0, 1) + part(1, 0)) + part(0, 0)
    )


def eliminate(matrix):
    size = matrix.shape[0]
    tiles = size // SUB
    row_ids = lax.broadcasted_iota(jnp.int32, (SUB, LANES), 0)
    columns = {}
    for j in range(size):
        for tile in range(j // SUB, tiles):
            part = matrix[tile * SUB : (tile + 1) * SUB, j : j + 1]
            columns[j, tile] = jnp.broadcast_to(part, (SUB, LANES))
    lanes = lane_ids((SUB, LANES))
    inverse = [jnp.where(lanes - tile * SUB == row_ids, 1.0, 0.0) for tile in range(tiles)]
    pivots = [jnp.ones((SUB, LANES), jnp.float32) for tile in range(tiles)]

    def pick(tile, row):
        return jnp.broadcast_to(tile[row : row + 1, :], (SUB, LANES))

    for k in range(size):
        home, place = k // SUB, k % SUB
        pivot = pick(columns[k, home], place)
        pivots[home] = jnp.where(row_ids == place, pivot, pivots[home])
        reciprocal = 1.0 / pivot
        factors = {}
        for tile in range(home, tiles):
            factors[tile] = columns[k, tile] * reciprocal
        factors[home] = jnp.where(row_ids > place, factors[home], 0.0)
        for j in range(k + 1, size):
            across = pick(columns[k, j // SUB], j % SUB)
            for tile in range(j // SUB, tiles):
                columns[j, tile] = columns[j, tile] - factors[tile] * across
        source = pick(inverse[home], place)
        for tile in range(home, tiles):
            inverse[tile] = inverse[tile] - factors[tile] * source
    lower = jnp.concatenate(inverse, axis=0)[:, :size]
    return lower, jnp.concatenate(pivots, axis=0)[:, :size]


def product(left, right, contract):
    return lax.dot_general(
        left, right, (contract, ((), ())), precision=HIGH, preferred_element_type=jnp.float32
    )


def modes_kernel(
    inputs, width_x, depth_y, scale,
    rank_ref, gram_ref, start_ref, direct_ref, adjoint_ref,
    direct_out, adjoint_out,
    direct_hold, sem,
):
    modes = start_ref.shape[0]

    ids = lax.broadcasted_iota(jnp.int32, (inputs, inputs), 0)
    chosen = jnp.where(rank_ref[0:1, :] == ids, 1.0, 0.0)
    start_sorted = product(chosen, start_ref[...], ((1,), (1,)))
    gram = gram_ref[...] * scale

    def orthonormal(block):
        lower, pivots = eliminate(product(block, block, ((0,), (0,))))
        return product(block, lower * lax.rsqrt(pivots), ((1,), (1,)))

    first = orthonormal(product(gram, start_sorted, ((1,), (0,))))
    right = orthonormal(product(gram, first, ((0,), (0,))))
    reached = product(gram, right, ((1,), (0,)))
    lower, pivots = eliminate(product(reached, reached, ((0,), (0,))))
    root = jnp.sqrt(pivots)
    quarter = jnp.sqrt(root)
    mixes = (
        product(lower / quarter, right, ((1,), (1,))),
        product(lower / (root * quarter), reached, ((1,), (1,))),
    )
    pairs = depth_y // 2
    for mix, source, out in zip(mixes, (direct_ref, adjoint_ref), (direct_hold, adjoint_out)):
        high, low, rest = split(mix)
        stacked = jnp.concatenate(
            [jnp.concatenate([high, high], axis=1), jnp.concatenate([low, low], axis=1)], axis=0
        )

        def project(pair, carry, stacked=stacked, source=source, out=out):
            both = jnp.dot(stacked, source[pair], preferred_element_type=jnp.float32)
            value = both[:modes] + both[modes:]
            for half in range(2):
                out[pl.ds(pair * 2 + half, modes, stride=width_x * depth_y), :] = value[
                    :, half * LANES : (half + 1) * LANES
                ]
            return carry

        lax.fori_loop(0, width_x * pairs, project, 0, unroll=8)
        if out is direct_hold:
            leave = pltpu.make_async_copy(direct_hold, direct_out, sem)
            leave.start()
    leave.wait()


def ordering(height):
    count = height.shape[0]
    at = lax.iota(jnp.int32, count)
    ahead = (height[None, :] < height[:, None]) | (
        (height[None, :] == height[:, None]) & (at[None, :] < at[:, None])
    )
    rank = jnp.sum(ahead.astype(jnp.int32), axis=1)
    ordered = jnp.sum(jnp.where(rank[None, :] == at[:, None], height[None, :], 0), axis=1)
    return rank, ordered


def everywhere(value, wide, narrow):
    axes = ("wide", "narrow")
    count = wide * narrow
    if count & (count - 1):
        return lax.psum(value, axes)
    bits = [narrow << i for i in range(wide.bit_length() - 1)]
    bits += [1 << i for i in range(narrow.bit_length() - 1)]

    def other(value, bit):
        return lax.ppermute(value, axes, [(i, i ^ bit) for i in range(count)])

    if bits:
        value = value + other(value, bits[0])
    rest = bits[1:]
    for at in range(0, len(rest), 2):
        pair = rest[at : at + 2]
        if len(pair) == 1:
            value = value + other(value, pair[0])
        else:
            first, second = pair
            value = (value + other(value, first)) + (other(value, second) + other(value, first ^ second))
    return value


def on_device(
    diffusivity,
    velocity,
    damping,
    input_amplitude,
    output_amplitude,
    input_height,
    output_height,
    start_block,
):
    inputs, width_x, width_z = input_amplitude.shape
    depth_y = diffusivity.shape[1]
    rank_count = start_block.shape[1]
    wide = lax.axis_size("wide")
    narrow = lax.axis_size("narrow")
    assert width_z == LANES and width_x == STEPS and inputs % (SUB * PER) == 0
    f32 = jnp.float32
    extent = 3 * width_x
    groups = inputs // SUB
    rims = groups // PER
    tiles = depth_y // SUB

    flat_in = input_amplitude.reshape(-1, width_z)
    flat_out = output_amplitude.reshape(-1, width_z)
    pieces = [flat_in, flat_out] + [
        cell.reshape(-1, width_z) for cell in (diffusivity, velocity, damping)
    ]
    sent = pl.pallas_call(
        stage_kernel,
        out_shape=jax.ShapeDtypeStruct((sum(piece.shape[0] for piece in pieces), width_z), f32),
        in_specs=[pl.BlockSpec(memory_space=pltpu.HBM)] * len(pieces),
        out_specs=VMEM,
        scratch_shapes=[pltpu.SemaphoreType.DMA((len(pieces),))],
        compiler_params=pltpu.CompilerParams(vmem_limit_bytes=60 * 1024 * 1024),
        name="stage",
    )(*pieces)
    near_pairs, far_pairs = swaps(wide)
    near = lax.ppermute(sent, "wide", near_pairs)
    far = lax.ppermute(sent, "wide", far_pairs)

    orders = [ordering(height) for height in (input_height, output_height)]
    ranks = jnp.stack([rank for rank, ordered in orders])
    heights = jnp.stack([ordered for rank, ordered in orders])
    by_group = heights.reshape(2, groups, SUB)
    by_rim = heights.reshape(2, rims, PER * SUB)
    bounds = jnp.concatenate(
        [
            jnp.stack([by_group[:, :, 0], by_group[:, :, -1]], axis=-1),
            jnp.stack([by_rim[:, :, 0], by_rim[:, :, -1]], axis=-1),
        ],
        axis=1,
    )
    rim_levels = heights.reshape(2, rims, PER, SUB).transpose(0, 1, 3, 2)
    levels = jnp.concatenate(
        [
            jnp.broadcast_to(heights[:, :, None], (2, inputs, LANES)),
            jnp.repeat(rim_levels, SLOT, axis=-1).reshape(2, rims * SUB, LANES),
        ],
        axis=1,
    )

    odd = lax.axis_index("wide") % 2
    place = jnp.stack([2 * width_x * (1 - odd), 2 * width_x * odd])
    rim_count = (2 * rims + -(-3 * tiles // PER)) * extent
    arranged, cells, rim = pl.pallas_call(
        functools.partial(pack_kernel, inputs, width_x, depth_y),
        out_shape=(
            jax.ShapeDtypeStruct((2, extent, inputs, LANES), f32),
            jax.ShapeDtypeStruct((3, extent, depth_y, LANES), f32),
            jax.ShapeDtypeStruct((rim_count, SUB, LANES), f32),
        ),
        in_specs=[SMEM, SMEM] + [VMEM] * 3,
        out_specs=(VMEM, VMEM, VMEM),
        compiler_params=pltpu.CompilerParams(vmem_limit_bytes=8 << 20),
        name="pack",
    )(place, ranks, sent, near, far)

    if narrow == 2:
        from_right = lax.ppermute(rim, "narrow", [(0, 1), (1, 0)])
        from_left = from_right
    else:
        from_right = lax.ppermute(rim, "narrow", [(i + 1, i) for i in range(narrow - 1)])
        from_left = lax.ppermute(rim, "narrow", [(i, i + 1) for i in range(narrow - 1)])
    side = lax.axis_index("narrow")
    flags = jnp.stack([(side + 1 < narrow).astype(jnp.int32), (side > 0).astype(jnp.int32)])

    pair_count = width_x * depth_y // 2
    cells_all = extent * depth_y
    field = pl.pallas_call(
        functools.partial(main_kernel, inputs, width_x, depth_y),
        out_shape=jax.ShapeDtypeStruct((2, width_x, depth_y, groups, SUB, LANES), f32),
        in_specs=[SMEM] + [VMEM] * 3,
        out_specs=VMEM,
        scratch_shapes=[
            pltpu.VMEM((4, extent, depth_y, SUB, LANES), f32),
            pltpu.VMEM((2 * groups, extent, depth_y + 2 * PAD, SUB, LANES), f32),
            pltpu.VMEM((2 * groups, extent, depth_y + 2 * PAD, SUB, LANES), f32),
        ],
        compiler_params=pltpu.CompilerParams(vmem_limit_bytes=46 << 20),
        cost_estimate=pl.CostEstimate(
            flops=2 * inputs * STEPS * cells_all * LANES * 12, bytes_accessed=6 << 20, transcendentals=0
        ),
        name="main",
    )(bounds, arranged, cells, levels)
    direct, adjoint, gram = pl.pallas_call(
        functools.partial(rim_kernel, inputs, width_x, depth_y),
        out_shape=(
            jax.ShapeDtypeStruct((pair_count, 2 * inputs, 2 * LANES), jnp.bfloat16),
            jax.ShapeDtypeStruct((pair_count, 2 * inputs, 2 * LANES), jnp.bfloat16),
            jax.ShapeDtypeStruct((inputs, inputs), f32),
        ),
        in_specs=[SMEM, SMEM] + [VMEM] * 5,
        out_specs=(VMEM, VMEM, VMEM),
        scratch_shapes=[
            pltpu.VMEM((2 * rims, extent, SUB, LANES), f32),
            pltpu.VMEM((4, extent, depth_y, SUB, LANES), f32),
            pltpu.VMEM((2 * rims, extent, depth_y + 2 * PAD, SUB, LANES), f32),
            pltpu.VMEM((2 * rims, extent, depth_y + 2 * PAD, SUB, LANES), f32),
            pltpu.VMEM((2 * rims, width_x, depth_y, SUB, LANES), f32),
            pltpu.VMEM((3 * inputs, 3 * inputs), f32),
        ],
        compiler_params=pltpu.CompilerParams(vmem_limit_bytes=22 << 20),
        name="rim",
    )(bounds, flags, rim, from_right, from_left, levels, field)

    gram = everywhere(gram, wide, narrow)

    scale = 1.0 / math.sqrt(width_x * wide * depth_y * width_z * narrow)
    shape = jax.ShapeDtypeStruct((rank_count * width_x * depth_y, LANES), f32)
    direct_modes, adjoint_modes = pl.pallas_call(
        functools.partial(modes_kernel, inputs, width_x, depth_y, scale),
        out_shape=(shape, shape),
        in_specs=[VMEM] * 5,
        out_specs=(pl.BlockSpec(memory_space=pltpu.HBM), VMEM),
        scratch_shapes=[pltpu.VMEM(shape.shape, f32), pltpu.SemaphoreType.DMA],
        compiler_params=pltpu.CompilerParams(vmem_limit_bytes=7 << 20),
        name="modes",
    )(ranks, gram, start_block.T, direct, adjoint)
    full = (rank_count, width_x, depth_y, width_z)
    return (direct_modes.reshape(full), adjoint_modes.reshape(full))


def solution(mesh):
    in_specs = (
        P("wide", None, "narrow"),
        P("wide", None, "narrow"),
        P("wide", None, "narrow"),
        P(None, "wide", "narrow"),
        P(None, "wide", "narrow"),
        P(),
        P(),
        P(),
    )
    out_specs = (P(None, "wide", None, "narrow"), P(None, "wide", None, "narrow"))
    return jax.shard_map(
        on_device, mesh=mesh, in_specs=in_specs, out_specs=out_specs, check_vma=False
    )
```

```python
import functools
import math

import jax
import jax.numpy as jnp
from jax import lax
from jax.experimental import pallas as pl
from jax.experimental.pallas import tpu as pltpu
from jax.sharding import PartitionSpec as P

STEPS = 4
HIGH = lax.Precision.HIGHEST
LANES = 128
SUB = 8
SLOT = 32
PER = LANES // SLOT
LEFT = 0
RIGHT = 16
REACH = STEPS + SUB
PAD = STEPS + 1

VMEM = pl.BlockSpec(memory_space=pltpu.VMEM)
SMEM = pl.BlockSpec(memory_space=pltpu.SMEM)


def swaps(count):
    near = [(i, i ^ 1) for i in range(count) if i ^ 1 < count]
    far = [(i, ((i + 1) ^ 1) - 1) for i in range(count) if 0 <= ((i + 1) ^ 1) - 1 < count]
    return near, far


def lane_ids(shape):
    return lax.broadcasted_iota(jnp.int32, shape, len(shape) - 1)


def turn(value, amount):
    return pltpu.roll(value, amount % LANES, value.ndim - 1)


def edges(block, slot):
    within = lane_ids(block.shape) - slot * SLOT
    low = turn(block, slot * SLOT + LEFT + STEPS)
    high = turn(block, slot * SLOT + RIGHT - (LANES - SUB))
    is_low = (within >= LEFT + STEPS) & (within < LEFT + REACH)
    is_high = (within >= RIGHT) & (within < RIGHT + SUB)
    return jnp.where(is_low, low, jnp.where(is_high, high, 0.0))


def stage_kernel(*refs):
    sources, target, sems = refs[:-2], refs[-2], refs[-1]
    copies = []
    at = 0
    for index, source in enumerate(sources):
        count = source.shape[0]
        copies.append(pltpu.make_async_copy(source, target.at[pl.ds(at, count)], sems.at[index]))
        at += count
    for copy in copies:
        copy.start()
    for copy in copies:
        copy.wait()


def rim_row(inputs, depth_y, sorted_ref, cell_ref, at):
    rims = inputs // SUB // PER
    values = []
    for system in range(2):
        for rim in range(rims):
            total = jnp.zeros((SUB, LANES), jnp.float32)
            for slot in range(PER):
                group = rim * PER + slot
                total = total + edges(sorted_ref[system, at, group * SUB : (group + 1) * SUB, :], slot)
            values.append(total)
    pieces = [(which, tile) for which in range(3) for tile in range(depth_y // SUB)]
    for first in range(0, len(pieces), PER):
        total = jnp.zeros((SUB, LANES), jnp.float32)
        for slot, (which, tile) in enumerate(pieces[first : first + PER]):
            total = total + edges(cell_ref[which, at, tile * SUB : (tile + 1) * SUB, :], slot)
        values.append(total)
    return values


def sort_rows(inputs, width_x, depth_y, rank_ref, sources, sorted_ref, cell_ref):
    for system in range(2):
        base = system * inputs * width_x

        def move(j, carry, system=system, base=base):
            to = rank_ref[system, j]
            for x in range(width_x):
                row = base + j * width_x + x
                for first, source in sources:
                    sorted_ref[system, first + x, pl.ds(to, 1), :] = source[pl.ds(row, 1), :]
            return carry

        lax.fori_loop(0, inputs, move, 0, unroll=8)
    start = 2 * inputs * width_x
    for which in range(3):
        for x in range(width_x):
            rows = pl.ds(start + (which * width_x + x) * depth_y, depth_y)
            for first, source in sources:
                cell_ref[which, first + x] = source[rows, :]


def own_kernel(inputs, width_x, depth_y, rank_ref, here, sorted_ref, cell_ref, rim_ref):
    sort_rows(inputs, width_x, depth_y, rank_ref, [(0, here)], sorted_ref, cell_ref)
    for x in range(width_x):
        for index, value in enumerate(rim_row(inputs, depth_y, sorted_ref, cell_ref, x)):
            rim_ref[index * width_x + x] = value


def pack_kernel(
    inputs, width_x, depth_y, place_ref, rank_ref, near, far, own_rim, sorted_ref, cell_ref, rim_ref
):
    sources = [(place_ref[0], near), (place_ref[1], far)]
    sort_rows(inputs, width_x, depth_y, rank_ref, sources, sorted_ref, cell_ref)
    extent = 3 * width_x
    for at in range(2 * width_x):
        x = at if at < width_x else at + width_x
        for index, value in enumerate(rim_row(inputs, depth_y, sorted_ref, cell_ref, at)):
            rim_ref[index * extent + x] = value
    for index in range(own_rim.shape[0] // width_x):
        for x in range(width_x):
            rim_ref[index * extent + width_x + x] = own_rim[index * width_x + x]


def split(value):
    first = value.astype(jnp.bfloat16)
    rest = value - first.astype(jnp.float32)
    second = rest.astype(jnp.bfloat16)
    third = (rest - second.astype(jnp.float32)).astype(jnp.bfloat16)
    return first, second, third


def store_cells(coef, x, tile, diff, vel, damp):
    inverse = jnp.where(diff > 0.0, 1.0 / jnp.where(diff > 0.0, diff, 1.0), 0.0)
    for which, value in enumerate((1.0 - 6.0 * diff - damp, diff, vel, inverse)):
        for y in range(SUB):
            coef[which, x, tile * SUB + y] = jnp.broadcast_to(value[y : y + 1, :], (SUB, LANES))


def march(units, share, depth_y, extent, bounds, load, heights, coef, ping, pong, write, wipe):
    zero = jnp.zeros((SUB, LANES), jnp.float32)
    count = len(units)
    low0 = [bounds[system, row, 0] for system, row in units]
    high0 = [bounds[system, row, 1] for system, row in units]
    top = depth_y - 1

    def begin(trip, carry):
        for at in range(count):
            y = jnp.minimum(low0[at] + trip, high0[at])
            here = heights(at) == y
            for x in range(extent):
                value = jnp.where(here, load(at, x), 0.0)
                if units[at][0]:
                    value = value * coef[1, x, y]
                ping[at, x, y + PAD] = value
        return carry

    most = functools.reduce(jnp.maximum, [high0[at] - low0[at] + 1 for at in range(count)])
    lax.fori_loop(0, most, begin, 0)
    for at in range(count):
        for x in range(extent):
            for buffer in (ping, pong):
                buffer[at, x, PAD - 1] = zero
                buffer[at, x, PAD + depth_y] = zero

        for x in range(1, extent - 1):
            ping[at, x, low0[at] - 1 + PAD] = zero
            ping[at, x, high0[at] + 1 + PAD] = zero

    for level in range(1, STEPS + 1):
        source, target = (ping, pong) if level % 2 else (pong, ping)
        low = [jnp.maximum(bound - level + 1, 0) for bound in low0]
        high = [jnp.minimum(bound + level - 1, top) for bound in high0]
        trips = functools.reduce(
            jnp.maximum, [(high[at] - low[at] + share) // share for at in range(count)]
        )

        def plane(at, y, level=level, source=source, target=target):
            system = units[at][0]
            rows = {}
            carried = {}
            for x in range(level - 1, extent - level + 1):
                rows[x] = source[at, x, y + PAD]
                if system:
                    carried[x] = rows[x] * coef[2, x, y]
            for x in range(level, extent - level):
                here = rows[x]
                behind, ahead = rows[x - 1], rows[x + 1]
                beside = (source[at, x, y + PAD - 1] + source[at, x, y + PAD + 1]) + (
                    turn(here, 1) + turn(here, -1)
                )
                if system:
                    drift = carried[x + 1] - carried[x - 1]
                else:
                    drift = coef[2, x, y] * (behind - ahead)
                total = beside + (behind + ahead) + drift
                if system and level == STEPS:
                    value = coef[0, x, y] * (here * coef[3, x, y]) + total
                else:
                    value = coef[0, x, y] * here + coef[1, x, y] * total
                if level == STEPS:
                    write(at, x - level, y, value)
                else:
                    target[at, x, y + PAD] = value

        def step(trip, carry, low=low, high=high, plane=plane):
            for at in range(count):
                for more in range(share):
                    plane(at, jnp.minimum(low[at] + (trip * share + more), high[at]))
            return carry

        lax.fori_loop(0, trips, step, 0)
        for at in range(count):
            for y, inner, outer in (
                (low0[at] - level, 1, -1),
                (high0[at] + level, -1, 1),
            ):
                inside = (y >= 0) & (y <= top)
                if level < STEPS:
                    near = jnp.minimum(jnp.maximum(y, 0), top)
                    for x in range(level, extent - level):
                        value = coef[1, x, near] * source[at, x, y + inner + PAD]
                        target[at, x, y + PAD] = jnp.where(inside, value, 0.0)
                        if level < x < extent - level - 1:
                            target[at, x, y + outer + PAD] = zero
                else:

                    @pl.when(inside)
                    def _(at=at, y=y, inner=inner, level=level, source=source):
                        for x in range(level, extent - level):
                            value = source[at, x, y + inner + PAD]
                            if not units[at][0]:
                                value = coef[1, x, y] * value
                            write(at, x - level, y, value)

            if level == STEPS:

                def clear(y, carry, at=at):
                    wipe(at, y, zero)
                    return carry

                lax.fori_loop(0, low0[at] - level, clear, 0)
                lax.fori_loop(high0[at] + level + 1, depth_y, clear, 0)


def main_kernel(
    inputs, width_x, depth_y, bounds_ref,
    own_sorted, own_cells, sorted_ref, cell_ref, level_ref, field, coef, ping, pong,
):
    groups = inputs // SUB
    extent = 3 * width_x

    def place(x, own, halo):
        if width_x <= x < 2 * width_x:
            return own, x - width_x
        return halo, x if x < width_x else x - width_x

    for x in range(extent):
        cells, at = place(x, own_cells, cell_ref)
        for tile in range(depth_y // SUB):
            rows = slice(tile * SUB, (tile + 1) * SUB)
            store_cells(coef, x, tile, *(cells[which, at, rows, :] for which in range(3)))
    units = [(system, group) for system in range(2) for group in range(groups)]

    def rows(at):
        return slice(units[at][1] * SUB, (units[at][1] + 1) * SUB)

    def write(at, x, y, value):
        field[units[at][0], x, y, units[at][1]] = value

    def wipe(at, y, zero):
        for x in range(width_x):
            write(at, x, y, zero)

    def load(at, x):
        source, index = place(x, own_sorted, sorted_ref)
        return source[units[at][0], index, rows(at), :]

    march(
        units, 1, depth_y, extent, bounds_ref,
        load,
        lambda at: level_ref[units[at][0], rows(at), :],
        coef, ping, pong, write, wipe,
    )


def rim_kernel(
    inputs, width_x, depth_y, bounds_ref, flag_ref,
    rim_ref, from_right, from_left, level_ref, field,
    direct_ref, adjoint_ref, gram_ref,
    amp, coef, ping, pong, edge_field, total_ref,
):
    groups = inputs // SUB
    rims = groups // PER
    extent = 3 * width_x
    tiles = depth_y // SUB
    lanes = lane_ids((SUB, LANES))
    within = lanes % SLOT
    from_right_lane = (within >= RIGHT + SUB) & (within < RIGHT + REACH) & (flag_ref[0] > 0)
    from_left_lane = (within >= LEFT) & (within < LEFT + STEPS) & (flag_ref[1] > 0)

    def whole_rim(index):
        value = rim_ref[index]
        value = jnp.where(from_right_lane, turn(from_right[index], RIGHT + SUB - STEPS), value)
        return jnp.where(from_left_lane, turn(from_left[index], LEFT - RIGHT - STEPS), value)

    pieces = [(which, tile) for which in range(3) for tile in range(tiles)]

    def prepare(x, carry):
        for system in range(2):
            for rim in range(rims):
                amp[system * rims + rim, x] = whole_rim((system * rims + rim) * extent + x)
        parts = {}
        for at in range(0, len(pieces), PER):
            packed = whole_rim((2 * rims + at // PER) * extent + x)
            for slot, piece in enumerate(pieces[at : at + PER]):
                alone = turn(jnp.where(lanes // SLOT == slot, packed, 0.0), -slot * SLOT)
                step = SLOT
                while step < LANES:
                    alone = alone + turn(alone, step)
                    step *= 2
                parts[piece] = alone
        for tile in range(tiles):
            store_cells(coef, x, tile, *(parts[(which, tile)] for which in range(3)))
        return carry

    lax.fori_loop(0, extent, prepare, 0, unroll=extent)
    units = [(system, groups + rim) for system in range(2) for rim in range(rims)]

    def rows(at):
        return slice(units[at][1] * SUB, (units[at][1] + 1) * SUB)

    def write(at, x, y, value):
        edge_field[at, x, y] = value

    def wipe(at, y, zero):
        for x in range(width_x):
            write(at, x, y, zero)

    march(
        units, 2, depth_y, extent, bounds_ref,
        lambda at, x: amp[at, x],
        lambda at: level_ref[units[at][0], rows(at), :],
        coef, ping, pong, write, wipe,
    )

    total_ref[...] = jnp.zeros_like(total_ref)
    pairs = depth_y // 2

    def fold(pair, carry):
        x = pair // pairs
        y = (pair % pairs) * 2
        stacked = []
        for system in range(2):
            halves = []
            for half in range(2):
                merged = []
                for rim in range(rims):
                    edge = edge_field[system * rims + rim, x, y + half]
                    edge = jnp.where(within < LEFT + STEPS, turn(edge, LEFT - RIGHT - STEPS), edge)
                    for slot in range(PER):
                        value = field[system, x, y + half, rim * PER + slot]
                        both = turn(edge, -(slot * SLOT + LEFT + STEPS))
                        outer = (lanes < STEPS) | (lanes >= LANES - STEPS)
                        merged.append(jnp.where(outer, both, value))
                halves.append(jnp.concatenate(merged, axis=0))
            whole = jnp.concatenate(halves, axis=1)
            first, second, third = split(whole)
            out = adjoint_ref if system else direct_ref
            out[pair, 0:inputs, :] = first
            out[pair, inputs : 2 * inputs, :] = second
            stacked.append(jnp.concatenate([first, second, third], axis=0))
        total_ref[...] += lax.dot_general(
            stacked[1], stacked[0], (((1,), (1,)), ((), ())), preferred_element_type=jnp.float32
        )
        return carry

    lax.fori_loop(0, width_x * pairs, fold, 0, unroll=4)

    def part(row, column):
        return total_ref[row * inputs : (row + 1) * inputs, column * inputs : (column + 1) * inputs]

    gram = (
        (part(0, 2) + part(2, 0)) + part(1, 1) + (part(0, 1) + part(1, 0)) + part(0, 0)
    )
    gram_ref[...] = jnp.concatenate([gram[: inputs // 2], gram[inputs // 2 :]], axis=1)


def eliminate(matrix):
    size = matrix.shape[0]
    tiles = size // SUB
    row_ids = lax.broadcasted_iota(jnp.int32, (SUB, LANES), 0)
    columns = {}
    for j in range(size):
        for tile in range(j // SUB, tiles):
            part = matrix[tile * SUB : (tile + 1) * SUB, j : j + 1]
            columns[j, tile] = jnp.broadcast_to(part, (SUB, LANES))
    lanes = lane_ids((SUB, LANES))
    inverse = [jnp.where(lanes - tile * SUB == row_ids, 1.0, 0.0) for tile in range(tiles)]
    pivots = [jnp.ones((SUB, LANES), jnp.float32) for tile in range(tiles)]

    def pick(tile, row):
        return jnp.broadcast_to(tile[row : row + 1, :], (SUB, LANES))

    for k in range(size):
        home, place = k // SUB, k % SUB
        pivot = pick(columns[k, home], place)
        pivots[home] = jnp.where(row_ids == place, pivot, pivots[home])
        reciprocal = 1.0 / pivot
        factors = {}
        for tile in range(home, tiles):
            factors[tile] = columns[k, tile] * reciprocal
        factors[home] = jnp.where(row_ids > place, factors[home], 0.0)
        for j in range(k + 1, size):
            across = pick(columns[k, j // SUB], j % SUB)
            for tile in range(j // SUB, tiles):
                columns[j, tile] = columns[j, tile] - factors[tile] * across
        source = pick(inverse[home], place)
        for tile in range(home, tiles):
            inverse[tile] = inverse[tile] - factors[tile] * source
    lower = jnp.concatenate(inverse, axis=0)[:, :size]
    return lower, jnp.concatenate(pivots, axis=0)[:, :size]


def product(left, right, contract):
    return lax.dot_general(
        left, right, (contract, ((), ())), precision=HIGH, preferred_element_type=jnp.float32
    )


def modes_kernel(
    inputs, width_x, depth_y, scale,
    rank_ref, gram_ref, start_ref, direct_ref, adjoint_ref,
    direct_out, adjoint_out,
    direct_hold, sem,
):
    modes = start_ref.shape[0]

    ids = lax.broadcasted_iota(jnp.int32, (inputs, inputs), 0)
    chosen = jnp.where(rank_ref[0:1, :] == ids, 1.0, 0.0)
    start_sorted = product(chosen, start_ref[...], ((1,), (1,)))
    gram = jnp.concatenate([gram_ref[:, :inputs], gram_ref[:, inputs:]], axis=0) * scale

    def orthonormal(block):
        lower, pivots = eliminate(product(block, block, ((0,), (0,))))
        return product(block, lower * lax.rsqrt(pivots), ((1,), (1,)))

    first = orthonormal(product(gram, start_sorted, ((1,), (0,))))
    right = orthonormal(product(gram, first, ((0,), (0,))))
    reached = product(gram, right, ((1,), (0,)))
    lower, pivots = eliminate(product(reached, reached, ((0,), (0,))))
    root = jnp.sqrt(pivots)
    quarter = jnp.sqrt(root)
    mixes = (
        product(lower / quarter, right, ((1,), (1,))),
        product(lower / (root * quarter), reached, ((1,), (1,))),
    )
    pairs = depth_y // 2
    for mix, source, out in zip(mixes, (direct_ref, adjoint_ref), (direct_hold, adjoint_out)):
        high, low, rest = split(mix)
        stacked = jnp.concatenate(
            [jnp.concatenate([high, high], axis=1), jnp.concatenate([low, low], axis=1)], axis=0
        )

        def project(pair, carry, stacked=stacked, source=source, out=out):
            both = jnp.dot(stacked, source[pair], preferred_element_type=jnp.float32)
            value = both[:modes] + both[modes:]
            for half in range(2):
                out[pl.ds(pair * 2 + half, modes, stride=width_x * depth_y), :] = value[
                    :, half * LANES : (half + 1) * LANES
                ]
            return carry

        lax.fori_loop(0, width_x * pairs, project, 0, unroll=8)
        if out is direct_hold:
            leave = pltpu.make_async_copy(direct_hold, direct_out, sem)
            leave.start()
    leave.wait()


def ordering(height):
    count = height.shape[0]
    at = lax.iota(jnp.int32, count)
    ahead = (height[None, :] < height[:, None]) | (
        (height[None, :] == height[:, None]) & (at[None, :] < at[:, None])
    )
    rank = jnp.sum(ahead.astype(jnp.int32), axis=1)
    ordered = jnp.sum(jnp.where(rank[None, :] == at[:, None], height[None, :], 0), axis=1)
    return rank, ordered


def everywhere(value, wide, narrow):
    axes = ("wide", "narrow")
    count = wide * narrow
    if count & (count - 1):
        return lax.psum(value, axes)
    bits = [narrow << i for i in range(wide.bit_length() - 1)]
    bits += [1 << i for i in range(narrow.bit_length() - 1)]

    def other(value, bit):
        return lax.ppermute(value, axes, [(i, i ^ bit) for i in range(count)])

    if bits:
        value = value + other(value, bits[0])
    rest = bits[1:]
    for at in range(0, len(rest), 2):
        pair = rest[at : at + 2]
        if len(pair) == 1:
            value = value + other(value, pair[0])
        else:
            first, second = pair
            value = (value + other(value, first)) + (other(value, second) + other(value, first ^ second))
    return value


def on_device(
    diffusivity,
    velocity,
    damping,
    input_amplitude,
    output_amplitude,
    input_height,
    output_height,
    start_block,
):
    inputs, width_x, width_z = input_amplitude.shape
    depth_y = diffusivity.shape[1]
    rank_count = start_block.shape[1]
    wide = lax.axis_size("wide")
    narrow = lax.axis_size("narrow")
    assert width_z == LANES and width_x == STEPS and inputs % (SUB * PER) == 0
    f32 = jnp.float32
    extent = 3 * width_x
    groups = inputs // SUB
    rims = groups // PER
    tiles = depth_y // SUB

    flat_in = input_amplitude.reshape(-1, width_z)
    flat_out = output_amplitude.reshape(-1, width_z)
    pieces = [flat_in, flat_out] + [
        cell.reshape(-1, width_z) for cell in (diffusivity, velocity, damping)
    ]
    sent = pl.pallas_call(
        stage_kernel,
        out_shape=jax.ShapeDtypeStruct((sum(piece.shape[0] for piece in pieces), width_z), f32),
        in_specs=[pl.BlockSpec(memory_space=pltpu.HBM)] * len(pieces),
        out_specs=VMEM,
        scratch_shapes=[pltpu.SemaphoreType.DMA((len(pieces),))],
        compiler_params=pltpu.CompilerParams(vmem_limit_bytes=60 * 1024 * 1024),
        name="stage",
    )(*pieces)
    near_pairs, far_pairs = swaps(wide)
    near = lax.ppermute(sent, "wide", near_pairs)
    far = lax.ppermute(sent, "wide", far_pairs)

    orders = [ordering(height) for height in (input_height, output_height)]
    ranks = jnp.stack([rank for rank, ordered in orders])
    heights = jnp.stack([ordered for rank, ordered in orders])
    by_group = heights.reshape(2, groups, SUB)
    by_rim = heights.reshape(2, rims, PER * SUB)
    bounds = jnp.concatenate(
        [
            jnp.stack([by_group[:, :, 0], by_group[:, :, -1]], axis=-1),
            jnp.stack([by_rim[:, :, 0], by_rim[:, :, -1]], axis=-1),
        ],
        axis=1,
    )
    rim_levels = heights.reshape(2, rims, PER, SUB).transpose(0, 1, 3, 2)
    levels = jnp.concatenate(
        [
            jnp.broadcast_to(heights[:, :, None], (2, inputs, LANES)),
            jnp.repeat(rim_levels, SLOT, axis=-1).reshape(2, rims * SUB, LANES),
        ],
        axis=1,
    )

    odd = lax.axis_index("wide") % 2
    place = jnp.stack([width_x * (1 - odd), width_x * odd])
    rim_kinds = 2 * rims + -(-3 * tiles // PER)
    own_sorted, own_cells, own_rim = pl.pallas_call(
        functools.partial(own_kernel, inputs, width_x, depth_y),
        out_shape=(
            jax.ShapeDtypeStruct((2, width_x, inputs, LANES), f32),
            jax.ShapeDtypeStruct((3, width_x, depth_y, LANES), f32),
            jax.ShapeDtypeStruct((rim_kinds * width_x, SUB, LANES), f32),
        ),
        in_specs=[SMEM, VMEM],
        out_specs=(VMEM, VMEM, VMEM),
        compiler_params=pltpu.CompilerParams(vmem_limit_bytes=8 << 20),
        cost_estimate=pl.CostEstimate(flops=1 << 22, bytes_accessed=1 << 20, transcendentals=0),
        name="own",
    )(ranks, sent)
    arranged, cells, rim = pl.pallas_call(
        functools.partial(pack_kernel, inputs, width_x, depth_y),
        out_shape=(
            jax.ShapeDtypeStruct((2, 2 * width_x, inputs, LANES), f32),
            jax.ShapeDtypeStruct((3, 2 * width_x, depth_y, LANES), f32),
            jax.ShapeDtypeStruct((rim_kinds * extent, SUB, LANES), f32),
        ),
        in_specs=[SMEM, SMEM] + [VMEM] * 3,
        out_specs=(VMEM, VMEM, VMEM),
        compiler_params=pltpu.CompilerParams(vmem_limit_bytes=8 << 20),
        name="pack",
    )(place, ranks, near, far, own_rim)

    if narrow == 2:
        from_right = lax.ppermute(rim, "narrow", [(0, 1), (1, 0)])
        from_left = from_right
    else:
        from_right = lax.ppermute(rim, "narrow", [(i + 1, i) for i in range(narrow - 1)])
        from_left = lax.ppermute(rim, "narrow", [(i, i + 1) for i in range(narrow - 1)])
    side = lax.axis_index("narrow")
    flags = jnp.stack([(side + 1 < narrow).astype(jnp.int32), (side > 0).astype(jnp.int32)])

    pair_count = width_x * depth_y // 2
    cells_all = extent * depth_y
    field = pl.pallas_call(
        functools.partial(main_kernel, inputs, width_x, depth_y),
        out_shape=jax.ShapeDtypeStruct((2, width_x, depth_y, groups, SUB, LANES), f32),
        in_specs=[SMEM] + [VMEM] * 5,
        out_specs=VMEM,
        scratch_shapes=[
            pltpu.VMEM((4, extent, depth_y, SUB, LANES), f32),
            pltpu.VMEM((2 * groups, extent, depth_y + 2 * PAD, SUB, LANES), f32),
            pltpu.VMEM((2 * groups, extent, depth_y + 2 * PAD, SUB, LANES), f32),
        ],
        compiler_params=pltpu.CompilerParams(vmem_limit_bytes=46 << 20),
        cost_estimate=pl.CostEstimate(
            flops=2 * inputs * STEPS * cells_all * LANES * 12, bytes_accessed=6 << 20, transcendentals=0
        ),
        name="main",
    )(bounds, own_sorted, own_cells, arranged, cells, levels)
    direct, adjoint, gram = pl.pallas_call(
        functools.partial(rim_kernel, inputs, width_x, depth_y),
        out_shape=(
            jax.ShapeDtypeStruct((pair_count, 2 * inputs, 2 * LANES), jnp.bfloat16),
            jax.ShapeDtypeStruct((pair_count, 2 * inputs, 2 * LANES), jnp.bfloat16),
            jax.ShapeDtypeStruct((inputs // 2, 2 * inputs), f32),
        ),
        in_specs=[SMEM, SMEM] + [VMEM] * 5,
        out_specs=(VMEM, VMEM, VMEM),
        scratch_shapes=[
            pltpu.VMEM((2 * rims, extent, SUB, LANES), f32),
            pltpu.VMEM((4, extent, depth_y, SUB, LANES), f32),
            pltpu.VMEM((2 * rims, extent, depth_y + 2 * PAD, SUB, LANES), f32),
            pltpu.VMEM((2 * rims, extent, depth_y + 2 * PAD, SUB, LANES), f32),
            pltpu.VMEM((2 * rims, width_x, depth_y, SUB, LANES), f32),
            pltpu.VMEM((3 * inputs, 3 * inputs), f32),
        ],
        compiler_params=pltpu.CompilerParams(vmem_limit_bytes=22 << 20),
        name="rim",
    )(bounds, flags, rim, from_right, from_left, levels, field)

    gram = everywhere(gram, wide, narrow)

    scale = 1.0 / math.sqrt(width_x * wide * depth_y * width_z * narrow)
    shape = jax.ShapeDtypeStruct((rank_count * width_x * depth_y, LANES), f32)
    direct_modes, adjoint_modes = pl.pallas_call(
        functools.partial(modes_kernel, inputs, width_x, depth_y, scale),
        out_shape=(shape, shape),
        in_specs=[VMEM] * 5,
        out_specs=(pl.BlockSpec(memory_space=pltpu.HBM), VMEM),
        scratch_shapes=[pltpu.VMEM(shape.shape, f32), pltpu.SemaphoreType.DMA],
        compiler_params=pltpu.CompilerParams(vmem_limit_bytes=7 << 20),
        name="modes",
    )(ranks, gram, start_block.T, direct, adjoint)
    full = (rank_count, width_x, depth_y, width_z)
    return (direct_modes.reshape(full), adjoint_modes.reshape(full))


def solution(mesh):
    in_specs = (
        P("wide", None, "narrow"),
        P("wide", None, "narrow"),
        P("wide", None, "narrow"),
        P(None, "wide", "narrow"),
        P(None, "wide", "narrow"),
        P(),
        P(),
        P(),
    )
    out_specs = (P(None, "wide", None, "narrow"), P(None, "wide", None, "narrow"))
    return jax.shard_map(
        on_device, mesh=mesh, in_specs=in_specs, out_specs=out_specs, check_vma=False
    )
```

```python
import functools
import math

import jax
import jax.numpy as jnp
from jax import lax
from jax.experimental import pallas as pl
from jax.experimental.pallas import tpu as pltpu
from jax.sharding import PartitionSpec as P

STEPS = 4
HIGH = lax.Precision.HIGHEST
LANES = 128
SUB = 8
SLOT = 32
PER = LANES // SLOT
LEFT = 0
RIGHT = 16
REACH = STEPS + SUB
PAD = STEPS + 1

VMEM = pl.BlockSpec(memory_space=pltpu.VMEM)
SMEM = pl.BlockSpec(memory_space=pltpu.SMEM)


def swaps(count):
    near = [(i, i ^ 1) for i in range(count) if i ^ 1 < count]
    far = [(i, ((i + 1) ^ 1) - 1) for i in range(count) if 0 <= ((i + 1) ^ 1) - 1 < count]
    return near, far


def lane_ids(shape):
    return lax.broadcasted_iota(jnp.int32, shape, len(shape) - 1)


def turn(value, amount):
    return pltpu.roll(value, amount % LANES, value.ndim - 1)


def edges(block, slot):
    within = lane_ids(block.shape) - slot * SLOT
    low = turn(block, slot * SLOT + LEFT + STEPS)
    high = turn(block, slot * SLOT + RIGHT - (LANES - SUB))
    is_low = (within >= LEFT + STEPS) & (within < LEFT + REACH)
    is_high = (within >= RIGHT) & (within < RIGHT + SUB)
    return jnp.where(is_low, low, jnp.where(is_high, high, 0.0))


def stage_kernel(*refs):
    sources, target, sems = refs[:-2], refs[-2], refs[-1]
    copies = []
    at = 0
    for index, source in enumerate(sources):
        count = source.shape[0]
        copies.append(pltpu.make_async_copy(source, target.at[pl.ds(at, count)], sems.at[index]))
        at += count
    for copy in copies:
        copy.start()
    for copy in copies:
        copy.wait()


def rim_row(inputs, depth_y, sorted_ref, cell_ref, at):
    rims = inputs // SUB // PER
    values = []
    for system in range(2):
        for rim in range(rims):
            total = jnp.zeros((SUB, LANES), jnp.float32)
            for slot in range(PER):
                group = rim * PER + slot
                total = total + edges(sorted_ref[system, at, group * SUB : (group + 1) * SUB, :], slot)
            values.append(total)
    pieces = [(which, tile) for which in range(3) for tile in range(depth_y // SUB)]
    for first in range(0, len(pieces), PER):
        total = jnp.zeros((SUB, LANES), jnp.float32)
        for slot, (which, tile) in enumerate(pieces[first : first + PER]):
            total = total + edges(cell_ref[which, at, tile * SUB : (tile + 1) * SUB, :], slot)
        values.append(total)
    return values


def sort_rows(inputs, width_x, depth_y, rank_ref, sources, sorted_ref, cell_ref):
    for system in range(2):
        base = system * inputs * width_x

        def move(j, carry, system=system, base=base):
            to = rank_ref[system, j]
            for x in range(width_x):
                row = base + j * width_x + x
                for first, source in sources:
                    sorted_ref[system, first + x, pl.ds(to, 1), :] = source[pl.ds(row, 1), :]
            return carry

        lax.fori_loop(0, inputs, move, 0, unroll=8)
    start = 2 * inputs * width_x
    for which in range(3):
        for x in range(width_x):
            rows = pl.ds(start + (which * width_x + x) * depth_y, depth_y)
            for first, source in sources:
                cell_ref[which, first + x] = source[rows, :]


def own_kernel(inputs, width_x, depth_y, rank_ref, here, sorted_ref, cell_ref, rim_ref):
    sort_rows(inputs, width_x, depth_y, rank_ref, [(0, here)], sorted_ref, cell_ref)
    for x in range(width_x):
        for index, value in enumerate(rim_row(inputs, depth_y, sorted_ref, cell_ref, x)):
            rim_ref[index * width_x + x] = value


def pack_kernel(
    inputs, width_x, depth_y, place_ref, rank_ref, near, far, own_rim, sorted_ref, cell_ref, rim_ref
):
    sources = [(place_ref[0], near), (place_ref[1], far)]
    sort_rows(inputs, width_x, depth_y, rank_ref, sources, sorted_ref, cell_ref)
    extent = 3 * width_x
    for at in range(2 * width_x):
        x = at if at < width_x else at + width_x
        for index, value in enumerate(rim_row(inputs, depth_y, sorted_ref, cell_ref, at)):
            rim_ref[index * extent + x] = value
    for index in range(own_rim.shape[0] // width_x):
        for x in range(width_x):
            rim_ref[index * extent + width_x + x] = own_rim[index * width_x + x]


def split(value):
    first = value.astype(jnp.bfloat16)
    rest = value - first.astype(jnp.float32)
    second = rest.astype(jnp.bfloat16)
    third = (rest - second.astype(jnp.float32)).astype(jnp.bfloat16)
    return first, second, third


def store_cells(coef, x, tile, diff, vel, damp):
    inverse = jnp.where(diff > 0.0, 1.0 / jnp.where(diff > 0.0, diff, 1.0), 0.0)
    for which, value in enumerate((1.0 - 6.0 * diff - damp, diff, vel, inverse)):
        for y in range(SUB):
            coef[which, x, tile * SUB + y] = jnp.broadcast_to(value[y : y + 1, :], (SUB, LANES))


def march(units, share, depth_y, extent, bounds, load, heights, coef, ping, pong, write, wipe):
    zero = jnp.zeros((SUB, LANES), jnp.float32)
    count = len(units)
    low0 = [bounds[system, row, 0] for system, row in units]
    high0 = [bounds[system, row, 1] for system, row in units]
    top = depth_y - 1
    per = count // 2
    span = max(share, 1)

    def begin(trip, carry):
        for at in range(count):
            y = jnp.minimum(low0[at] + trip, high0[at])
            here = heights(at) == y
            for x in range(extent):
                value = jnp.where(here, load(at, x), 0.0)
                if units[at][0]:
                    value = value * coef[1, x, y]
                ping[at, x, y + PAD] = value
        return carry

    most = functools.reduce(jnp.maximum, [high0[at] - low0[at] + 1 for at in range(count)])
    lax.fori_loop(0, most, begin, 0)
    for at in range(count):
        for x in range(extent):
            for buffer in (ping, pong):
                buffer[at, x, PAD - 1] = zero
                buffer[at, x, PAD + depth_y] = zero

        for x in range(1, extent - 1):
            ping[at, x, low0[at] - 1 + PAD] = zero
            ping[at, x, high0[at] + 1 + PAD] = zero

    for level in range(1, STEPS + 1):
        source, target = (ping, pong) if level % 2 else (pong, ping)
        low = [jnp.maximum(bound - level + 1, 0) for bound in low0]
        high = [jnp.minimum(bound + level - 1, top) for bound in high0]
        trips = functools.reduce(
            jnp.maximum, [(high[at] - low[at] + span) // span for at in range(count)]
        )

        def plane(system, row, y, level=level, source=source, target=target):
            at = system * per + row
            rows = {}
            carried = {}
            for x in range(level - 1, extent - level + 1):
                rows[x] = source[at, x, y + PAD]
                if system:
                    carried[x] = rows[x] * coef[2, x, y]
            for x in range(level, extent - level):
                here = rows[x]
                behind, ahead = rows[x - 1], rows[x + 1]
                beside = (source[at, x, y + PAD - 1] + source[at, x, y + PAD + 1]) + (
                    turn(here, 1) + turn(here, -1)
                )
                if system:
                    drift = carried[x + 1] - carried[x - 1]
                else:
                    drift = coef[2, x, y] * (behind - ahead)
                total = beside + (behind + ahead) + drift
                if system and level == STEPS:
                    value = coef[0, x, y] * (here * coef[3, x, y]) + total
                else:
                    value = coef[0, x, y] * here + coef[1, x, y] * total
                if level == STEPS:
                    write(system, row, x - level, y, value)
                else:
                    target[at, x, y + PAD] = value

        if share:

            def step(trip, carry, low=low, high=high, plane=plane):
                for at in range(count):
                    for more in range(share):
                        y = jnp.minimum(low[at] + (trip * share + more), high[at])
                        plane(units[at][0], at % per, y)
                return carry

        else:
            ends, bases = [], []
            for at in range(count):
                before = 0 if at % per == 0 else ends[-1]
                bases.append(low[at] - before)
                ends.append(before + high[at] - low[at] + 1)
            trips = (jnp.maximum(ends[per - 1], ends[count - 1]) + per - 1) // per

            def step(trip, carry, ends=ends, bases=bases, plane=plane):
                for system in range(2):
                    first = system * per
                    for more in range(per):
                        place = jnp.minimum(trip * per + more, ends[first + per - 1] - 1)
                        row, base = 0, bases[first]
                        for other in range(per - 1):
                            later = place >= ends[first + other]
                            row = jnp.where(later, other + 1, row)
                            base = jnp.where(later, bases[first + other + 1], base)
                        plane(system, row, place + base)
                return carry

        lax.fori_loop(0, trips, step, 0)
        for at in range(count):
            for y, inner, outer in (
                (low0[at] - level, 1, -1),
                (high0[at] + level, -1, 1),
            ):
                inside = (y >= 0) & (y <= top)
                if level < STEPS:
                    near = jnp.minimum(jnp.maximum(y, 0), top)
                    for x in range(level, extent - level):
                        value = coef[1, x, near] * source[at, x, y + inner + PAD]
                        target[at, x, y + PAD] = jnp.where(inside, value, 0.0)
                        if level < x < extent - level - 1:
                            target[at, x, y + outer + PAD] = zero
                else:

                    @pl.when(inside)
                    def _(at=at, y=y, inner=inner, level=level, source=source):
                        for x in range(level, extent - level):
                            value = source[at, x, y + inner + PAD]
                            if not units[at][0]:
                                value = coef[1, x, y] * value
                            write(units[at][0], at % per, x - level, y, value)

            if level == STEPS:

                def clear(y, carry, at=at):
                    wipe(at, y, zero)
                    return carry

                lax.fori_loop(0, low0[at] - level, clear, 0)
                lax.fori_loop(high0[at] + level + 1, depth_y, clear, 0)


def main_kernel(
    inputs, width_x, depth_y, bounds_ref,
    own_sorted, own_cells, sorted_ref, cell_ref, level_ref, field, coef, ping, pong,
):
    groups = inputs // SUB
    extent = 3 * width_x

    def place(x, own, halo):
        if width_x <= x < 2 * width_x:
            return own, x - width_x
        return halo, x if x < width_x else x - width_x

    for x in range(extent):
        cells, at = place(x, own_cells, cell_ref)
        for tile in range(depth_y // SUB):
            rows = slice(tile * SUB, (tile + 1) * SUB)
            store_cells(coef, x, tile, *(cells[which, at, rows, :] for which in range(3)))
    units = [(system, group) for system in range(2) for group in range(groups)]

    def rows(at):
        return slice(units[at][1] * SUB, (units[at][1] + 1) * SUB)

    def write(system, row, x, y, value):
        field[system, x, y, row] = value

    def wipe(at, y, zero):
        for x in range(width_x):
            write(units[at][0], units[at][1], x, y, zero)

    def load(at, x):
        source, index = place(x, own_sorted, sorted_ref)
        return source[units[at][0], index, rows(at), :]

    march(
        units, 0, depth_y, extent, bounds_ref,
        load,
        lambda at: level_ref[units[at][0], rows(at), :],
        coef, ping, pong, write, wipe,
    )


def rim_kernel(
    inputs, width_x, depth_y, bounds_ref, flag_ref,
    rim_ref, from_right, from_left, level_ref, field,
    direct_ref, adjoint_ref, gram_ref,
    amp, coef, ping, pong, edge_field, total_ref,
):
    groups = inputs // SUB
    rims = groups // PER
    extent = 3 * width_x
    tiles = depth_y // SUB
    lanes = lane_ids((SUB, LANES))
    within = lanes % SLOT
    from_right_lane = (within >= RIGHT + SUB) & (within < RIGHT + REACH) & (flag_ref[0] > 0)
    from_left_lane = (within >= LEFT) & (within < LEFT + STEPS) & (flag_ref[1] > 0)

    def whole_rim(index):
        value = rim_ref[index]
        value = jnp.where(from_right_lane, turn(from_right[index], RIGHT + SUB - STEPS), value)
        return jnp.where(from_left_lane, turn(from_left[index], LEFT - RIGHT - STEPS), value)

    pieces = [(which, tile) for which in range(3) for tile in range(tiles)]

    def prepare(x, carry):
        for system in range(2):
            for rim in range(rims):
                amp[system * rims + rim, x] = whole_rim((system * rims + rim) * extent + x)
        parts = {}
        for at in range(0, len(pieces), PER):
            packed = whole_rim((2 * rims + at // PER) * extent + x)
            for slot, piece in enumerate(pieces[at : at + PER]):
                alone = turn(jnp.where(lanes // SLOT == slot, packed, 0.0), -slot * SLOT)
                step = SLOT
                while step < LANES:
                    alone = alone + turn(alone, step)
                    step *= 2
                parts[piece] = alone
        for tile in range(tiles):
            store_cells(coef, x, tile, *(parts[(which, tile)] for which in range(3)))
        return carry

    lax.fori_loop(0, extent, prepare, 0, unroll=extent)
    units = [(system, groups + rim) for system in range(2) for rim in range(rims)]

    def rows(at):
        return slice(units[at][1] * SUB, (units[at][1] + 1) * SUB)

    def write(system, row, x, y, value):
        edge_field[system * rims + row, x, y] = value

    def wipe(at, y, zero):
        for x in range(width_x):
            edge_field[at, x, y] = zero

    march(
        units, 3, depth_y, extent, bounds_ref,
        lambda at, x: amp[at, x],
        lambda at: level_ref[units[at][0], rows(at), :],
        coef, ping, pong, write, wipe,
    )

    total_ref[...] = jnp.zeros_like(total_ref)
    pairs = depth_y // 2

    def fold(pair, carry):
        x = pair // pairs
        y = (pair % pairs) * 2
        stacked = []
        for system in range(2):
            halves = []
            for half in range(2):
                merged = []
                for rim in range(rims):
                    edge = edge_field[system * rims + rim, x, y + half]
                    edge = jnp.where(within < LEFT + STEPS, turn(edge, LEFT - RIGHT - STEPS), edge)
                    for slot in range(PER):
                        value = field[system, x, y + half, rim * PER + slot]
                        both = turn(edge, -(slot * SLOT + LEFT + STEPS))
                        outer = (lanes < STEPS) | (lanes >= LANES - STEPS)
                        merged.append(jnp.where(outer, both, value))
                halves.append(jnp.concatenate(merged, axis=0))
            whole = jnp.concatenate(halves, axis=1)
            first, second, third = split(whole)
            out = adjoint_ref if system else direct_ref
            out[pair, 0:inputs, :] = first
            out[pair, inputs : 2 * inputs, :] = second
            stacked.append(jnp.concatenate([first, second, third], axis=0))
        total_ref[...] += lax.dot_general(
            stacked[1], stacked[0], (((1,), (1,)), ((), ())), preferred_element_type=jnp.float32
        )
        return carry

    lax.fori_loop(0, width_x * pairs, fold, 0, unroll=8)

    def part(row, column):
        return total_ref[row * inputs : (row + 1) * inputs, column * inputs : (column + 1) * inputs]

    gram = (
        (part(0, 2) + part(2, 0)) + part(1, 1) + (part(0, 1) + part(1, 0)) + part(0, 0)
    )
    gram_ref[...] = jnp.concatenate([gram[: inputs // 2], gram[inputs // 2 :]], axis=1)


def eliminate(matrix):
    size = matrix.shape[0]
    tiles = size // SUB
    row_ids = lax.broadcasted_iota(jnp.int32, (SUB, LANES), 0)
    columns = {}
    for j in range(size):
        for tile in range(j // SUB, tiles):
            part = matrix[tile * SUB : (tile + 1) * SUB, j : j + 1]
            columns[j, tile] = jnp.broadcast_to(part, (SUB, LANES))
    lanes = lane_ids((SUB, LANES))
    inverse = [jnp.where(lanes - tile * SUB == row_ids, 1.0, 0.0) for tile in range(tiles)]
    pivots = [jnp.ones((SUB, LANES), jnp.float32) for tile in range(tiles)]

    def pick(tile, row):
        return jnp.broadcast_to(tile[row : row + 1, :], (SUB, LANES))

    for k in range(size):
        home, place = k // SUB, k % SUB
        pivot = pick(columns[k, home], place)
        pivots[home] = jnp.where(row_ids == place, pivot, pivots[home])
        reciprocal = 1.0 / pivot
        factors = {}
        for tile in range(home, tiles):
            factors[tile] = columns[k, tile] * reciprocal
        factors[home] = jnp.where(row_ids > place, factors[home], 0.0)
        for j in range(k + 1, size):
            across = pick(columns[k, j // SUB], j % SUB)
            for tile in range(j // SUB, tiles):
                columns[j, tile] = columns[j, tile] - factors[tile] * across
        source = pick(inverse[home], place)
        for tile in range(home, tiles):
            inverse[tile] = inverse[tile] - factors[tile] * source
    lower = jnp.concatenate(inverse, axis=0)[:, :size]
    return lower, jnp.concatenate(pivots, axis=0)[:, :size]


def product(left, right, contract):
    return lax.dot_general(
        left, right, (contract, ((), ())), precision=HIGH, preferred_element_type=jnp.float32
    )


def modes_kernel(
    inputs, width_x, depth_y, scale,
    rank_ref, gram_ref, start_ref, direct_ref, adjoint_ref,
    direct_out, adjoint_out,
    direct_hold, sem,
):
    modes = start_ref.shape[0]

    ids = lax.broadcasted_iota(jnp.int32, (inputs, inputs), 0)
    chosen = jnp.where(rank_ref[0:1, :] == ids, 1.0, 0.0)
    start_sorted = product(chosen, start_ref[...], ((1,), (1,)))
    gram = jnp.concatenate([gram_ref[:, :inputs], gram_ref[:, inputs:]], axis=0) * scale

    def orthonormal(block):
        lower, pivots = eliminate(product(block, block, ((0,), (0,))))
        return product(block, lower * lax.rsqrt(pivots), ((1,), (1,)))

    first = orthonormal(product(gram, start_sorted, ((1,), (0,))))
    right = orthonormal(product(gram, first, ((0,), (0,))))
    reached = product(gram, right, ((1,), (0,)))
    lower, pivots = eliminate(product(reached, reached, ((0,), (0,))))
    root = jnp.sqrt(pivots)
    quarter = jnp.sqrt(root)
    mixes = (
        product(lower / quarter, right, ((1,), (1,))),
        product(lower / (root * quarter), reached, ((1,), (1,))),
    )
    pairs = depth_y // 2
    for mix, source, out in zip(mixes, (direct_ref, adjoint_ref), (direct_hold, adjoint_out)):
        high, low, rest = split(mix)
        stacked = jnp.concatenate(
            [jnp.concatenate([high, high], axis=1), jnp.concatenate([low, low], axis=1)], axis=0
        )

        def project(pair, carry, stacked=stacked, source=source, out=out):
            both = jnp.dot(stacked, source[pair], preferred_element_type=jnp.float32)
            value = both[:modes] + both[modes:]
            for half in range(2):
                out[pl.ds(pair * 2 + half, modes, stride=width_x * depth_y), :] = value[
                    :, half * LANES : (half + 1) * LANES
                ]
            return carry

        lax.fori_loop(0, width_x * pairs, project, 0, unroll=16)
        if out is direct_hold:
            leave = pltpu.make_async_copy(direct_hold, direct_out, sem)
            leave.start()
    leave.wait()


def ordering(height):
    count = height.shape[0]
    at = lax.iota(jnp.int32, count)
    ahead = (height[None, :] < height[:, None]) | (
        (height[None, :] == height[:, None]) & (at[None, :] < at[:, None])
    )
    rank = jnp.sum(ahead.astype(jnp.int32), axis=1)
    ordered = jnp.sum(jnp.where(rank[None, :] == at[:, None], height[None, :], 0), axis=1)
    return rank, ordered


def everywhere(value, wide, narrow):
    axes = ("wide", "narrow")
    count = wide * narrow
    if count & (count - 1):
        return lax.psum(value, axes)
    bits = [narrow << i for i in range(wide.bit_length() - 1)]
    bits += [1 << i for i in range(narrow.bit_length() - 1)]

    def other(value, bit):
        return lax.ppermute(value, axes, [(i, i ^ bit) for i in range(count)])

    if bits:
        value = value + other(value, bits[0])
    rest = bits[1:]
    for at in range(0, len(rest), 2):
        pair = rest[at : at + 2]
        if len(pair) == 1:
            value = value + other(value, pair[0])
        else:
            first, second = pair
            value = (value + other(value, first)) + (other(value, second) + other(value, first ^ second))
    return value


def on_device(
    diffusivity,
    velocity,
    damping,
    input_amplitude,
    output_amplitude,
    input_height,
    output_height,
    start_block,
):
    inputs, width_x, width_z = input_amplitude.shape
    depth_y = diffusivity.shape[1]
    rank_count = start_block.shape[1]
    wide = lax.axis_size("wide")
    narrow = lax.axis_size("narrow")
    assert width_z == LANES and width_x == STEPS and inputs % (SUB * PER) == 0
    f32 = jnp.float32
    extent = 3 * width_x
    groups = inputs // SUB
    rims = groups // PER
    tiles = depth_y // SUB

    flat_in = input_amplitude.reshape(-1, width_z)
    flat_out = output_amplitude.reshape(-1, width_z)
    pieces = [flat_in, flat_out] + [
        cell.reshape(-1, width_z) for cell in (diffusivity, velocity, damping)
    ]
    sent = pl.pallas_call(
        stage_kernel,
        out_shape=jax.ShapeDtypeStruct((sum(piece.shape[0] for piece in pieces), width_z), f32),
        in_specs=[pl.BlockSpec(memory_space=pltpu.HBM)] * len(pieces),
        out_specs=VMEM,
        scratch_shapes=[pltpu.SemaphoreType.DMA((len(pieces),))],
        compiler_params=pltpu.CompilerParams(vmem_limit_bytes=60 * 1024 * 1024),
        name="stage",
    )(*pieces)
    near_pairs, far_pairs = swaps(wide)
    near = lax.ppermute(sent, "wide", near_pairs)
    far = lax.ppermute(sent, "wide", far_pairs)

    orders = [ordering(height) for height in (input_height, output_height)]
    ranks = jnp.stack([rank for rank, ordered in orders])
    heights = jnp.stack([ordered for rank, ordered in orders])
    by_group = heights.reshape(2, groups, SUB)
    by_rim = heights.reshape(2, rims, PER * SUB)
    bounds = jnp.concatenate(
        [
            jnp.stack([by_group[:, :, 0], by_group[:, :, -1]], axis=-1),
            jnp.stack([by_rim[:, :, 0], by_rim[:, :, -1]], axis=-1),
        ],
        axis=1,
    )
    rim_levels = heights.reshape(2, rims, PER, SUB).transpose(0, 1, 3, 2)
    levels = jnp.concatenate(
        [
            jnp.broadcast_to(heights[:, :, None], (2, inputs, LANES)),
            jnp.repeat(rim_levels, SLOT, axis=-1).reshape(2, rims * SUB, LANES),
        ],
        axis=1,
    )

    odd = lax.axis_index("wide") % 2
    place = jnp.stack([width_x * (1 - odd), width_x * odd])
    rim_kinds = 2 * rims + -(-3 * tiles // PER)
    own_sorted, own_cells, own_rim = pl.pallas_call(
        functools.partial(own_kernel, inputs, width_x, depth_y),
        out_shape=(
            jax.ShapeDtypeStruct((2, width_x, inputs, LANES), f32),
            jax.ShapeDtypeStruct((3, width_x, depth_y, LANES), f32),
            jax.ShapeDtypeStruct((rim_kinds * width_x, SUB, LANES), f32),
        ),
        in_specs=[SMEM, VMEM],
        out_specs=(VMEM, VMEM, VMEM),
        compiler_params=pltpu.CompilerParams(vmem_limit_bytes=8 << 20),
        cost_estimate=pl.CostEstimate(flops=1 << 22, bytes_accessed=1 << 20, transcendentals=0),
        name="own",
    )(ranks, sent)
    arranged, cells, rim = pl.pallas_call(
        functools.partial(pack_kernel, inputs, width_x, depth_y),
        out_shape=(
            jax.ShapeDtypeStruct((2, 2 * width_x, inputs, LANES), f32),
            jax.ShapeDtypeStruct((3, 2 * width_x, depth_y, LANES), f32),
            jax.ShapeDtypeStruct((rim_kinds * extent, SUB, LANES), f32),
        ),
        in_specs=[SMEM, SMEM] + [VMEM] * 3,
        out_specs=(VMEM, VMEM, VMEM),
        compiler_params=pltpu.CompilerParams(vmem_limit_bytes=8 << 20),
        name="pack",
    )(place, ranks, near, far, own_rim)

    if narrow == 2:
        from_right = lax.ppermute(rim, "narrow", [(0, 1), (1, 0)])
        from_left = from_right
    else:
        from_right = lax.ppermute(rim, "narrow", [(i + 1, i) for i in range(narrow - 1)])
        from_left = lax.ppermute(rim, "narrow", [(i, i + 1) for i in range(narrow - 1)])
    side = lax.axis_index("narrow")
    flags = jnp.stack([(side + 1 < narrow).astype(jnp.int32), (side > 0).astype(jnp.int32)])

    pair_count = width_x * depth_y // 2
    cells_all = extent * depth_y
    field = pl.pallas_call(
        functools.partial(main_kernel, inputs, width_x, depth_y),
        out_shape=jax.ShapeDtypeStruct((2, width_x, depth_y, groups, SUB, LANES), f32),
        in_specs=[SMEM] + [VMEM] * 5,
        out_specs=VMEM,
        scratch_shapes=[
            pltpu.VMEM((4, extent, depth_y, SUB, LANES), f32),
            pltpu.VMEM((2 * groups, extent, depth_y + 2 * PAD, SUB, LANES), f32),
            pltpu.VMEM((2 * groups, extent, depth_y + 2 * PAD, SUB, LANES), f32),
        ],
        compiler_params=pltpu.CompilerParams(vmem_limit_bytes=46 << 20),
        cost_estimate=pl.CostEstimate(
            flops=2 * inputs * STEPS * cells_all * LANES * 12, bytes_accessed=6 << 20, transcendentals=0
        ),
        name="main",
    )(bounds, own_sorted, own_cells, arranged, cells, levels)
    direct, adjoint, gram = pl.pallas_call(
        functools.partial(rim_kernel, inputs, width_x, depth_y),
        out_shape=(
            jax.ShapeDtypeStruct((pair_count, 2 * inputs, 2 * LANES), jnp.bfloat16),
            jax.ShapeDtypeStruct((pair_count, 2 * inputs, 2 * LANES), jnp.bfloat16),
            jax.ShapeDtypeStruct((inputs // 2, 2 * inputs), f32),
        ),
        in_specs=[SMEM, SMEM] + [VMEM] * 5,
        out_specs=(VMEM, VMEM, VMEM),
        scratch_shapes=[
            pltpu.VMEM((2 * rims, extent, SUB, LANES), f32),
            pltpu.VMEM((4, extent, depth_y, SUB, LANES), f32),
            pltpu.VMEM((2 * rims, extent, depth_y + 2 * PAD, SUB, LANES), f32),
            pltpu.VMEM((2 * rims, extent, depth_y + 2 * PAD, SUB, LANES), f32),
            pltpu.VMEM((2 * rims, width_x, depth_y, SUB, LANES), f32),
            pltpu.VMEM((3 * inputs, 3 * inputs), f32),
        ],
        compiler_params=pltpu.CompilerParams(vmem_limit_bytes=22 << 20),
        name="rim",
    )(bounds, flags, rim, from_right, from_left, levels, field)

    gram = everywhere(gram, wide, narrow)

    scale = 1.0 / math.sqrt(width_x * wide * depth_y * width_z * narrow)
    shape = jax.ShapeDtypeStruct((rank_count * width_x * depth_y, LANES), f32)
    direct_modes, adjoint_modes = pl.pallas_call(
        functools.partial(modes_kernel, inputs, width_x, depth_y, scale),
        out_shape=(shape, shape),
        in_specs=[VMEM] * 5,
        out_specs=(pl.BlockSpec(memory_space=pltpu.HBM), VMEM),
        scratch_shapes=[pltpu.VMEM(shape.shape, f32), pltpu.SemaphoreType.DMA],
        compiler_params=pltpu.CompilerParams(vmem_limit_bytes=7 << 20),
        name="modes",
    )(ranks, gram, start_block.T, direct, adjoint)
    full = (rank_count, width_x, depth_y, width_z)
    return (direct_modes.reshape(full), adjoint_modes.reshape(full))


def solution(mesh):
    in_specs = (
        P("wide", None, "narrow"),
        P("wide", None, "narrow"),
        P("wide", None, "narrow"),
        P(None, "wide", "narrow"),
        P(None, "wide", "narrow"),
        P(),
        P(),
        P(),
    )
    out_specs = (P(None, "wide", None, "narrow"), P(None, "wide", None, "narrow"))
    return jax.shard_map(
        on_device, mesh=mesh, in_specs=in_specs, out_specs=out_specs, check_vma=False
    )
```
